256 devices in a mesh: ep: 16 (over y, z_lo, core), etp: 16 (over z_hi, x).
Axes of the slice: x: 4, y: 4, z: 8 (z_hi: 4, z_lo: 2; z = z_hi * 2 + z_lo), core: 2. Of those that a mesh axis runs over, the one named last changes fastest.
Arguments:
- tokens: bfloat16 [32768, 7168], P(('ep', 'etp')), may hold values from -6 to 6
- expert_ids: int32 [32768, 8], P(('ep', 'etp')), may hold values from 0 to 383, all different within a row; in each aligned block of 128 rows (0 to 127, 128 to 255, ...) at most 3 rows name the same one
- gate_q: int32 [32768, 8], P(('ep', 'etp')), may hold values from 1 to 1024
- w_gate: bfloat16 [16, 7168, 2048], P('ep', None, 'etp'), may hold values from -0.0625 to 0.0625
- w_up: bfloat16 [16, 7168, 2048], P('ep', None, 'etp'), may hold values from -0.0625 to 0.0625
- w_down: bfloat16 [16, 2048, 7168], P('ep', 'etp'), may hold values from -0.125 to 0.125
Outputs:
- mixed: bfloat16 [32768, 7168], P(('ep', 'etp'))
The draws below stay inside these ranges and needn't reach their ends.
Inputs may be any that keep to these rules, and one draw needn't show every extreme that they name: `expert_ids`: each row names 8 different experts; among the 128 rows of one device no expert is named by more than 3 rows.
All inputs are finite; a program needn't handle non-finite values.
Results may differ from the reference program's by a relative error of at most 0.014.
Values may be sent and summed in bfloat16 or wider, within the bound.
A program may use at most 64 MiB of HBM per device.

```python
import math
import jax
import jax.numpy as jnp
import numpy as np
from jax import lax

D = 7168
FF = 2048
EXPERTS_ALL = 384
TOP = 8
TOK_DEV = 128
CAP = 3
EXPERTS_WIN = 16
TOKENS = 32768
N_EP = 16
N_ETP = 16
DEVICES = 256


def plant(entries, stream_key, smallest, largest):
    place = [jax.random.randint(jax.random.fold_in(stream_key, axis), (), 0, length) for axis, length in enumerate(entries.shape)]
    main_axis = entries.shape.index(max(entries.shape))
    next_to = place[:main_axis] + [(place[main_axis] + 1) % entries.shape[main_axis]] + place[main_axis + 1:]
    return entries.at[tuple(place)].set(smallest).at[tuple(next_to)].set(largest)


def block_scale(own_key, extent, split, smallest, largest):
    def one(position, blocks):
        draws = jax.random.uniform(jax.random.fold_in(jax.random.fold_in(own_key, 6), position), (blocks,), jnp.float32, smallest / len(split), largest / len(split))
        return jnp.repeat(jnp.exp(draws), extent[position] // blocks).reshape((-1,) + (1,) * (len(extent) - position - 1))

    loudness = one(*split[0])
    for cut in split[1:]:
        loudness = loudness * one(*cut)
    return loudness


def deal_out(key, own, number, rows, number_of, top, limit, lean):
    sequence = jax.random.permutation(key, number_of)
    heavy_load, ordinary = portions_of(number_of, rows * top, limit, lean, True), portions_of(number_of, rows * top, limit, lean, False)
    places = jnp.arange(number_of)

    def named(sizes, offset_by):
        used = int((sizes > 0).sum())
        fixed = max(1, used // 4)
        shifted = fixed + (places - fixed + offset_by * (used - fixed)) % max(1, number_of - fixed)
        return jnp.zeros((number_of,), jnp.int32).at[sequence[jnp.where(places < fixed, places, shifted)]].set(jnp.asarray(sizes, jnp.int32))

    sizes = jnp.where(number % 4 == 0, named(heavy_load, number // 4), named(ordinary, number - number // 4 - 1))
    mixed = jax.random.permutation(jax.random.fold_in(own, 3), number_of)
    donor, receiver = mixed[0:number_of // 2 * 2:2], mixed[1:number_of // 2 * 2:2]
    room = jnp.minimum(sizes[donor] - 1, limit - sizes[receiver]) // 2
    room = jnp.where((donor == sequence[0]) | (receiver == sequence[0]) | (sizes[receiver] == 0), 0, jnp.maximum(room, 0))
    shifted = jax.random.randint(jax.random.fold_in(own, 4), (number_of // 2,), 0, 1 << 20) % (room + 1)
    sizes = sizes.at[donor].add(-shifted).at[receiver].add(shifted)
    items = jnp.searchsorted(jnp.cumsum(sizes), jnp.arange(rows * top), side="right").astype(jnp.int32)
    listing = items.reshape(top, rows).T
    listing = listing[jax.random.permutation(jax.random.fold_in(own, 1), rows)]
    offset_by = jax.random.randint(jax.random.fold_in(own, 2), (rows, 1), 0, top)
    return jnp.take_along_axis(listing, (jnp.arange(top)[None, :] + offset_by) % top, axis=1)


def portions_of(count, total, reach, lean, full):
    loads = [(1 << 20) // math.isqrt(standing ** lean) + 1 for standing in range(1, count + 1)]
    largest = reach if full else min(reach, max(-(-total // count), total * loads[0] // sum(loads)))
    least = 1 if total - largest >= count - 1 else 0
    holding, surplus = [largest] + [least] * (count - 1), total - largest - least * (count - 1)
    while surplus > 0:
        candidates = [i for i in range(1, count) if holding[i] < largest] or [i for i in range(1, count) if holding[i] < reach]
        mass, left = sum([loads[i] for i in candidates]), surplus
        for i in candidates:
            addition = min(reach - holding[i], max(1, left * loads[i] // mass), surplus)
            holding[i] = holding[i] + addition
            surplus = surplus - addition
    return np.array(holding)


def bell_draw(stream_key, shape, spread, reach, cuts=(), kind=jnp.bfloat16):
    values = jax.random.normal(stream_key, shape, jnp.float32) * spread
    if len(cuts) > 0:
        values = block_scale(stream_key, shape, cuts, -0.22, 0.18) * values
    return jnp.clip(values, min=-reach, max=reach).astype(kind)


def setup_inputs(seed: int = 0) -> dict:
    keys = jax.random.split(jax.random.key(seed), 7)
    tokens = bell_draw(keys[0], (TOKENS, D), 1.0, 6.0, ((0, 256),))
    expert_ids_keys = jax.random.split(jax.random.fold_in(keys[1], 1), TOKENS // TOK_DEV)
    expert_ids_turns = jax.random.permutation(jax.random.fold_in(keys[1], 3), TOKENS // TOK_DEV)
    expert_ids = jax.vmap(lambda own, number: deal_out(jax.random.fold_in(keys[1], 2), own, number, TOK_DEV, EXPERTS_ALL, TOP, CAP, 2))(expert_ids_keys, expert_ids_turns).reshape((TOKENS, TOP))
    gate_q = plant(jax.random.randint(keys[2], (TOKENS, TOP), 1, 1025), jax.random.fold_in(keys[2], 1), 1, 1024).astype(jnp.int32)
    w_gate = bell_draw(keys[3], (EXPERTS_WIN, D, FF), D ** -0.5, 0.0625, ((0, 16), (2, 16)))
    w_up = bell_draw(keys[4], (EXPERTS_WIN, D, FF), D ** -0.5, 0.0625, ((0, 16), (2, 16)))
    w_down = bell_draw(keys[5], (EXPERTS_WIN, FF, D), FF ** -0.5, 0.125, ((0, 16), (1, 16)))
    return dict(tokens=tokens, expert_ids=expert_ids, gate_q=gate_q, w_gate=w_gate, w_up=w_up, w_down=w_down)


def reference(tokens, expert_ids, gate_q, w_gate, w_up, w_down):
    slots = DEVICES * CAP
    group = FF // N_ETP
    weights = gate_q.astype(jnp.float32) / 1024.0

    def one_expert(carry, expert):
        match = expert_ids == expert
        token_weight = jnp.sum(jnp.where(match, weights, jnp.float32(0.0)), axis=1)
        used = jnp.any(match, axis=1)
        index = jnp.nonzero(used, size=slots, fill_value=0)[0].astype(jnp.int32)
        valid = jnp.arange(slots, dtype=jnp.int32) < jnp.sum(used.astype(jnp.int32))
        rows = tokens[index]
        gate = jnp.dot(rows, w_gate[expert], preferred_element_type=jnp.float32)
        upper = jnp.dot(rows, w_up[expert], preferred_element_type=jnp.float32)
        hidden = (jax.nn.silu(gate) * upper).astype(jnp.bfloat16)
        hidden_groups = hidden.reshape(slots, N_ETP, group).transpose(1, 0, 2)
        down_groups = w_down[expert].reshape(N_ETP, group, D)

        def add_group(total, pair):
            part = jnp.dot(pair[0], pair[1], preferred_element_type=jnp.float32).astype(jnp.bfloat16)
            return total + part.astype(jnp.float32), None

        summed, _ = lax.scan(add_group, jnp.zeros((slots, D), jnp.float32), (hidden_groups, down_groups))
        expert_out = summed.astype(jnp.bfloat16).astype(jnp.float32)
        scale = jnp.where(valid, token_weight[index], jnp.float32(0.0))
        carry = carry.at[index].add(scale[:, None] * expert_out)
        return carry, None

    total, _ = lax.scan(one_expert, jnp.zeros((TOKENS, D), jnp.float32), jnp.arange(N_EP, dtype=jnp.int32))
    return total.astype(jnp.bfloat16)
```

```python
import functools

import jax
import jax.numpy as jnp
import numpy as np
from jax import lax
from jax.experimental import pallas as pl
from jax.experimental.pallas import tpu as pltpu
from jax.sharding import PartitionSpec as P

CAP = 3
RING = 4
MESH = pl.DeviceIdType.MESH
F32 = jnp.float32
BF16 = jnp.bfloat16


def third(c):
    return lax.shift_right_logical(c * 43691, 17)


def kernel(ids_ref, gate_ref, p1_ref, p1t_ref, p2_ref, p2t_ref, tok_hbm, wg_hbm, wu_hbm, wd_hbm,
           ret_ref, scal_ref,
           tok, bs, xa, sb, rb, X, wgu, wd, gp, own, hr, H, pown, pfar, pnear, pcomb, rfar, rdir, rcomb,
           sr, rr, ts,
           loc_sem, w_send, w_recv, a_send, a_recv, b_send, b_recv, z_send, z_recv, g_send, g_recv,
           h_send, h_recv, r_send, r_recv, c_send, c_recv, d_send, d_recv):
    ep = lax.axis_index("ep")
    etp = lax.axis_index("etp")
    n_ep = lax.axis_size("ep")
    zi = etp // RING
    x = etp % RING
    width = tok.shape[1]
    D4 = width // RING
    slots = n_ep * CAP
    R = slots * RING
    half = R // 2
    inner = wd.shape[0] // RING

    def xdev(k):
        return (ep, zi * RING + lax.rem(x + k, RING))

    def zdev(k):
        return (ep, lax.rem(zi + k, RING) * RING + x)

    def edev(k):
        return (lax.rem(ep + k, n_ep), etp)

    def send(src, dst, ssem, rsem, dev):
        c = pltpu.make_async_remote_copy(src_ref=src, dst_ref=dst, send_sem=ssem, recv_sem=rsem,
                                         device_id=dev, device_id_type=MESH)
        c.start()
        return c

    def rows(start, size):
        return pl.ds(pl.multiple_of(start, 16), size)

    def cols(start, size):
        return pl.ds(pl.multiple_of(start, 128), size)

    tok_copy = pltpu.make_async_copy(tok_hbm, tok, loc_sem.at[0])
    tok_copy.start()
    w_loc = [
        pltpu.make_async_copy(wg_hbm.at[0, rows(x * D4, D4), :], wgu.at[x, :, pl.ds(0, inner)], loc_sem.at[1]),
        pltpu.make_async_copy(wu_hbm.at[0, rows(x * D4, D4), :], wgu.at[x, :, pl.ds(inner, inner)], loc_sem.at[2]),
        pltpu.make_async_copy(wd_hbm.at[0, :, cols(x * D4, D4)], wd.at[rows(x * inner, inner), :], loc_sem.at[3]),
    ]

    barrier = pltpu.get_barrier_semaphore()
    for k in range(1, RING):
        pl.semaphore_signal(barrier, inc=1, device_id=xdev(k), device_id_type=MESH)
    for k in (1, RING - 1):
        pl.semaphore_signal(barrier, inc=1, device_id=zdev(k), device_id_type=MESH)
    for k in range(1, n_ep):
        pl.semaphore_signal(barrier, inc=1, device_id=edev(k), device_id_type=MESH)

    T = tok.shape[0]
    c = lax.broadcasted_iota(jnp.int32, (slots, T), 0)
    expert = third(c)
    slot = (c - CAP * expert).astype(F32)
    hot = jnp.zeros((slots, T), F32)
    weight = jnp.zeros((slots, T), F32)
    for r in range(ids_ref.shape[0]):
        eq = ids_ref[r:r + 1, :] == expert
        hot = jnp.where(eq, 1.0, hot)
        weight = jnp.where(eq, gate_ref[r:r + 1, :].astype(F32), weight)
    before = lax.broadcasted_iota(jnp.int32, (T, T), 0) < lax.broadcasted_iota(jnp.int32, (T, T), 1)
    earlier = jnp.dot(hot.astype(BF16), jnp.where(before, 1.0, 0.0).astype(BF16), preferred_element_type=F32)
    placing = jnp.where(earlier == slot, hot, 0.0)
    scal_ref[...] = placing * weight * (1.0 / 1024.0)
    placing = placing.astype(BF16)

    tok_copy.wait()
    pl.semaphore_wait(barrier, (RING - 1) + 2 + (n_ep - 1))

    a_copies = []
    for k in (2, 1, 3, 0):
        dst_x = lax.rem(x + k, RING)
        piece = jnp.dot(placing, tok[:, cols(dst_x * D4, D4)], preferred_element_type=F32).astype(BF16)
        if k == 0:
            xa[rows(x * slots, slots), :] = piece
        else:
            bs[k - 1] = piece
            a_copies.append(send(bs.at[k - 1], xa.at[rows(x * slots, slots), :], a_send.at[k - 1], a_recv.at[k - 1], xdev(k)))

    w_copies = []
    for i, k in enumerate((1, 3, 2)):
        dst_x = lax.rem(x + k, RING)
        w_copies.append(send(wg_hbm.at[0, rows(dst_x * D4, D4), :], wgu.at[x, :, pl.ds(0, inner)],
                             w_send.at[0, i], w_recv.at[0, i], xdev(k)))
        w_copies.append(send(wu_hbm.at[0, rows(dst_x * D4, D4), :], wgu.at[x, :, pl.ds(inner, inner)],
                             w_send.at[1, i], w_recv.at[1, i], xdev(k)))
    d_copies = []
    for i, k in enumerate((1, 3, 2)):
        dst_x = lax.rem(x + k, RING)
        d_copies.append(send(wd_hbm.at[0, :, cols(dst_x * D4, D4)], wd.at[rows(x * inner, inner), :],
                             w_send.at[2, i], w_recv.at[2, i], xdev(k)))
    for cp in w_loc:
        cp.start()

    for cp in a_copies:
        cp.wait_recv()

    sb[...] = jnp.dot(p1_ref[...], xa[...], preferred_element_type=F32).astype(BF16)
    b_copies = []
    for k in range(1, n_ep):
        dst_e = lax.rem(ep + k, n_ep)
        b_copies.append(send(sb.at[rows(dst_e * 16, 16), :], rb.at[rows(ep * 16, 16), :],
                             b_send.at[k - 1], b_recv.at[k - 1], edev(k)))
    rb[rows(ep * 16, 16), :] = sb[rows(ep * 16, 16), :]
    for cp in b_copies:
        cp.wait_recv()
    X[rows(zi * R, R), :] = jnp.dot(p2_ref[...], rb[...], preferred_element_type=F32).astype(BF16)

    zm = lax.rem(zi + RING - 1, RING)
    zp = lax.rem(zi + 1, RING)
    zf = lax.rem(zi + 2, RING)

    def zsend(block, lo, i, k):
        part = X.at[rows(block * R + (0 if lo else half), half), :]
        return send(part, part, z_send.at[i], z_recv.at[i], zdev(k))

    zc = [None] * 6
    zc[0] = zsend(zi, True, 0, 1)
    zc[3] = zsend(zi, False, 3, RING - 1)
    zc[1] = zsend(zi, False, 1, 1)
    zc[4] = zsend(zi, True, 4, RING - 1)
    zc[0].wait_recv()
    zc[2] = zsend(zm, True, 2, 1)
    zc[3].wait_recv()
    zc[5] = zsend(zp, False, 5, RING - 1)

    for cp in w_copies:
        cp.wait_recv()
    w_loc[0].wait()
    w_loc[1].wait()

    order = [zi, zm, zp, zf]
    g_copies = [[None] * (RING - 1) for _ in range(4)]
    h_copies = [[None] * (RING - 1) for _ in range(4)]

    def first(i):
        b = order[i]
        xs = X[rows(b * R, R), :]
        for k in (2, 1, 3, 0):
            dst_x = lax.rem(x + k, RING)
            acc = jnp.dot(xs, wgu[dst_x], preferred_element_type=F32)
            if k == 0:
                own[i] = acc
            else:
                gp[i, k - 1] = acc.astype(BF16)
                g_copies[i][k - 1] = send(gp.at[i, k - 1], hr.at[i, k - 1], g_send.at[i, k - 1],
                                          g_recv.at[i, k - 1], xdev(k))

    def second(i):
        b = order[i]
        total = own[i]
        for k in range(RING - 1):
            g_copies[i][k].wait_recv()
            total = total + hr[i, k].astype(F32)
        g = total[:, :inner]
        u = total[:, inner:]
        H[rows(b * R, R), cols(x * inner, inner)] = (g / (1.0 + jnp.exp(-g)) * u).astype(BF16)
        for k in range(1, RING):
            part = H.at[rows(b * R, R), cols(x * inner, inner)]
            h_copies[i][k - 1] = send(part, part, h_send.at[i, k - 1], h_recv.at[i, k - 1], xdev(k))

    def third_(i):
        b = order[i]
        for k in range(RING - 1):
            h_copies[i][k].wait_recv()
        return jnp.dot(H[rows(b * R, R), :], wd[...], preferred_element_type=F32)

    first(0)
    zc[1].wait_recv()
    first(1)
    zc[4].wait_recv()
    first(2)
    second(0)
    second(1)
    zc[2].wait_recv()
    zc[5].wait_recv()
    first(3)
    second(2)
    second(3)
    for cp in d_copies:
        cp.wait_recv()
    w_loc[2].wait()

    def rsend(src, dst, i, k):
        return send(src, dst, r_send.at[i], r_recv.at[i], zdev(k))

    lo, hi = slice(0, half), slice(half, R)
    rc = [None] * 6
    far = third_(3)
    pfar[...] = far.astype(BF16)
    rc[0] = rsend(pfar.at[pl.ds(0, half), :], rfar.at[0], 0, 1)
    rc[3] = rsend(pfar.at[pl.ds(half, half), :], rfar.at[1], 3, RING - 1)
    up = third_(2)
    pnear[0] = up[hi].astype(BF16)
    pcomb[0] = up[lo].astype(BF16)
    rc[1] = rsend(pnear.at[0], rdir.at[0], 1, 1)
    down = third_(1)
    pnear[1] = down[lo].astype(BF16)
    pcomb[1] = down[hi].astype(BF16)
    rc[4] = rsend(pnear.at[1], rdir.at[1], 4, RING - 1)
    pown[...] = third_(0)
    rc[0].wait_recv()
    pcomb[0] = (pcomb[0].astype(F32) + rfar[0].astype(F32)).astype(BF16)
    rc[2] = rsend(pcomb.at[0], rcomb.at[0], 2, 1)
    rc[3].wait_recv()
    pcomb[1] = (pcomb[1].astype(F32) + rfar[1].astype(F32)).astype(BF16)
    rc[5] = rsend(pcomb.at[1], rcomb.at[1], 5, RING - 1)
    rc[1].wait_recv()
    rc[4].wait_recv()
    rc[2].wait_recv()
    rc[5].wait_recv()
    y_lo = pown[pl.ds(0, half), :] + rcomb[0].astype(F32) + rdir[1].astype(F32)
    y_hi = pown[pl.ds(half, half), :] + rcomb[1].astype(F32) + rdir[0].astype(F32)
    y = jnp.concatenate([y_lo.astype(BF16), y_hi.astype(BF16)], axis=0)

    sr[...] = jnp.dot(p2t_ref[...], y, preferred_element_type=F32).astype(BF16)
    cc = []
    for k in range(1, n_ep):
        dst_e = lax.rem(ep + k, n_ep)
        cc.append(send(sr.at[rows(dst_e * 16, 16), :], rr.at[rows(ep * 16, 16), :],
                       c_send.at[k - 1], c_recv.at[k - 1], edev(k)))
    rr[rows(ep * 16, 16), :] = sr[rows(ep * 16, 16), :]
    for cp in cc:
        cp.wait_recv()
    ts[...] = jnp.dot(p1t_ref[...], rr[...], preferred_element_type=F32).astype(BF16)
    dc = []
    for k in range(1, RING):
        dst_x = lax.rem(x + k, RING)
        dc.append(send(ts.at[rows(dst_x * slots, slots), :], ret_ref.at[:, cols(x * D4, D4)],
                       d_send.at[k - 1], d_recv.at[k - 1], xdev(k)))
    ret_ref[:, cols(x * D4, D4)] = ts[rows(x * slots, slots), :]
    for cp in dc:
        cp.wait_recv()
    for group in [a_copies, w_copies, d_copies, b_copies, zc, rc, cc, dc] + g_copies + h_copies:
        for cp in group:
            cp.wait_send()


def body(tokens, expert_ids, gate_q, w_gate, w_up, w_down):
    n_ep = lax.axis_size("ep")
    T, width = tokens.shape
    D4 = width // RING
    slots = n_ep * CAP
    R = slots * RING
    inner = w_down.shape[1]
    per = CAP * RING

    p1 = np.zeros((n_ep * 16, R), np.float32)
    p2 = np.zeros((R, n_ep * 16), np.float32)
    for e in range(n_ep):
        for s in range(RING):
            for q in range(CAP):
                p1[e * 16 + s * CAP + q, s * slots + e * CAP + q] = 1
        for j in range(per):
            p2[e * per + j, e * 16 + j] = 1
    consts = [jnp.asarray(m, BF16) for m in (p1, p1.T, p2, p2.T)]

    vm = pl.BlockSpec(memory_space=pltpu.VMEM)
    anyspec = pl.BlockSpec(memory_space=pl.ANY)
    V = pltpu.VMEM
    DMA = pltpu.SemaphoreType.DMA
    half = R // 2
    scratch = [
        V((T, width), BF16),
        V((3, slots, D4), BF16),
        V((R, D4), BF16),
        V((n_ep * 16, D4), BF16),
        V((n_ep * 16, D4), BF16),
        V((RING * R, D4), BF16),
        V((RING, D4, 2 * inner), BF16),
        V((RING * inner, D4), BF16),
        V((RING, 3, R, 2 * inner), BF16),
        V((RING, R, 2 * inner), F32),
        V((RING, 3, R, 2 * inner), BF16),
        V((RING * R, RING * inner), BF16),
        V((R, D4), F32),
        V((R, D4), BF16),
        V((2, half, D4), BF16),
        V((2, half, D4), BF16),
        V((2, half, D4), BF16),
        V((2, half, D4), BF16),
        V((2, half, D4), BF16),
        V((n_ep * 16, D4), BF16),
        V((n_ep * 16, D4), BF16),
        V((R, D4), BF16),
        DMA((4,)), DMA((3, 3)), DMA((3, 3)), DMA((3,)), DMA((3,)),
        DMA((n_ep - 1,)), DMA((n_ep - 1,)), DMA((6,)), DMA((6,)),
        DMA((4, 3)), DMA((4, 3)), DMA((4, 3)), DMA((4, 3)), DMA((6,)), DMA((6,)),
        DMA((n_ep - 1,)), DMA((n_ep - 1,)), DMA((3,)), DMA((3,)),
    ]
    ret, scal = pl.pallas_call(
        kernel,
        out_shape=(jax.ShapeDtypeStruct((slots, width), BF16), jax.ShapeDtypeStruct((slots, T), F32)),
        in_specs=[vm] * 6 + [anyspec] * 4,
        out_specs=(vm, vm),
        scratch_shapes=scratch,
        compiler_params=pltpu.CompilerParams(collective_id=0, has_side_effects=True, vmem_limit_bytes=60 * 1024 * 1024),
        name="experts",
    )(expert_ids.T, gate_q.T, *consts, tokens, w_gate, w_up, w_down)
    mixed = lax.dot_general(scal, ret.astype(F32), (((0,), (0,)), ((), ())))
    return mixed.astype(BF16)


def solution(mesh):
    in_specs = (
        P(("ep", "etp"), None),
        P(("ep", "etp"), None),
        P(("ep", "etp"), None),
        P("ep", None, "etp"),
        P("ep", None, "etp"),
        P("ep", "etp", None),
    )
    out_specs = P(("ep", "etp"), None)
    return jax.shard_map(body, mesh=mesh, in_specs=in_specs, out_specs=out_specs, check_vma=False)
```

```python
import jax
import jax.numpy as jnp
import numpy as np
from jax import lax
from jax.experimental import pallas as pl
from jax.experimental.pallas import tpu as pltpu
from jax.sharding import PartitionSpec as P

CAP = 3
RING = 4
C = 2
MESH = pl.DeviceIdType.MESH
F32 = jnp.float32
BF16 = jnp.bfloat16
scope = jax.named_scope


def third(c):
    return lax.shift_right_logical(c * 43691, 17)


def dot(a, b):
    return jnp.dot(a, b, preferred_element_type=F32)


def kernel(ids_ref, gate_ref, p1_ref, p1t_ref, p2_ref, p2t_ref, tok_hbm, wg_hbm, wu_hbm, wd_hbm,
           ret_ref, scal_ref,
           tok, bs, xa, sb, rb, X, wgu, wd, gp, own, hr, H, pown, pfar, pnear, pcomb, rfar, rdir, rcomb,
           sr, rr, ts,
           loc_sem, w_send, w_recv, a_send, a_recv, b_send, b_recv, z_send, z_recv, g_send, g_recv,
           h_send, h_recv, r_send, r_recv, c_send, c_recv, d_send, d_recv):
    ep = lax.axis_index("ep")
    etp = lax.axis_index("etp")
    n_ep = lax.axis_size("ep")
    zi = etp // RING
    x = etp % RING
    width = tok.shape[1]
    D4 = width // RING
    DC = D4 // C
    slots = n_ep * CAP
    R = slots * RING
    half = R // 2
    inner = wd.shape[1] // RING

    def xdev(k):
        return (ep, zi * RING + lax.rem(x + k, RING))

    def zdev(k):
        return (ep, lax.rem(zi + k, RING) * RING + x)

    def edev(k):
        return (lax.rem(ep + k, n_ep), etp)

    everything = []

    def send(src, dst, ssem, rsem, dev):
        c = pltpu.make_async_remote_copy(src_ref=src, dst_ref=dst, send_sem=ssem, recv_sem=rsem,
                                         device_id=dev, device_id_type=MESH)
        c.start()
        everything.append(c)
        return c

    def rows(start, size):
        return pl.ds(pl.multiple_of(start, 16), size)

    def cols(start, size):
        return pl.ds(pl.multiple_of(start, 128), size)

    tok_copy = pltpu.make_async_copy(tok_hbm, tok, loc_sem.at[0])
    tok_copy.start()
    w_loc = [
        pltpu.make_async_copy(wg_hbm.at[0, rows(x * D4, D4), :], wgu.at[x, :, pl.ds(0, inner)], loc_sem.at[1]),
        pltpu.make_async_copy(wu_hbm.at[0, rows(x * D4, D4), :], wgu.at[x, :, pl.ds(inner, inner)], loc_sem.at[2]),
    ] + [
        pltpu.make_async_copy(wd_hbm.at[0, :, cols(x * D4 + q * DC, DC)], wd.at[q, rows(x * inner, inner), :], loc_sem.at[3 + q])
        for q in range(C)
    ]

    barrier = pltpu.get_barrier_semaphore()
    for k in range(1, RING):
        pl.semaphore_signal(barrier, inc=1, device_id=xdev(k), device_id_type=MESH)
    for k in (1, RING - 1):
        pl.semaphore_signal(barrier, inc=1, device_id=zdev(k), device_id_type=MESH)
    for k in range(1, n_ep):
        pl.semaphore_signal(barrier, inc=1, device_id=edev(k), device_id_type=MESH)

    T = tok.shape[0]
    c = lax.broadcasted_iota(jnp.int32, (slots, T), 0)
    expert = third(c)
    slot = (c - CAP * expert).astype(F32)
    hot = jnp.zeros((slots, T), F32)
    weight = jnp.zeros((slots, T), F32)
    for r in range(ids_ref.shape[0]):
        eq = ids_ref[r:r + 1, :] == expert
        hot = jnp.where(eq, 1.0, hot)
        weight = jnp.where(eq, gate_ref[r:r + 1, :].astype(F32), weight)
    before = lax.broadcasted_iota(jnp.int32, (T, T), 0) < lax.broadcasted_iota(jnp.int32, (T, T), 1)
    earlier = dot(hot.astype(BF16), jnp.where(before, 1.0, 0.0).astype(BF16))
    placing = jnp.where(earlier == slot, hot, 0.0)
    scal_ref[...] = placing * weight * (1.0 / 1024.0)
    placing = placing.astype(BF16)

    with scope("tokwait"):
        tok_copy.wait()
    with scope("barrier_in"):
        pl.semaphore_wait(barrier, (RING - 1) + 2 + (n_ep - 1))

    a_copies = [[], []]
    for q in range(C):
        for k in (2, 1, 3, 0):
            dst_x = lax.rem(x + k, RING)
            piece = dot(placing, tok[:, cols(dst_x * D4 + q * DC, DC)]).astype(BF16)
            if k == 0:
                xa[q, rows(x * slots, slots), :] = piece
            else:
                bs[q, k - 1] = piece
                a_copies[q].append(send(bs.at[q, k - 1], xa.at[q, rows(x * slots, slots), :],
                                        a_send.at[q, k - 1], a_recv.at[q, k - 1], xdev(k)))

    w_copies = []
    for i, k in enumerate((1, 3, 2)):
        dst_x = lax.rem(x + k, RING)
        w_copies.append(send(wg_hbm.at[0, rows(dst_x * D4, D4), :], wgu.at[x, :, pl.ds(0, inner)],
                             w_send.at[0, i], w_recv.at[0, i], xdev(k)))
        w_copies.append(send(wu_hbm.at[0, rows(dst_x * D4, D4), :], wgu.at[x, :, pl.ds(inner, inner)],
                             w_send.at[1, i], w_recv.at[1, i], xdev(k)))

    def send_down(q):
        out = []
        for i, k in enumerate((1, 3, 2)):
            dst_x = lax.rem(x + k, RING)
            out.append(send(wd_hbm.at[0, :, cols(dst_x * D4 + q * DC, DC)],
                            wd.at[q, rows(x * inner, inner), :],
                            w_send.at[2 + q, i], w_recv.at[2 + q, i], xdev(k)))
        return out

    d_copies = [send_down(0)]
    for cp in w_loc:
        cp.start()

    b_copies = [[], []]
    for q in range(C):
        with scope("A_wait"):
            for cp in a_copies[q]:
                cp.wait_recv()
        sb[q] = dot(p1_ref[...], xa[q]).astype(BF16)
        for k in range(1, n_ep):
            dst_e = lax.rem(ep + k, n_ep)
            b_copies[q].append(send(sb.at[q, rows(dst_e * 16, 16), :], rb.at[q, rows(ep * 16, 16), :],
                                    b_send.at[q, k - 1], b_recv.at[q, k - 1], edev(k)))
        rb[q, rows(ep * 16, 16), :] = sb[q, rows(ep * 16, 16), :]

    zm = lax.rem(zi + RING - 1, RING)
    zp = lax.rem(zi + 1, RING)
    zf = lax.rem(zi + 2, RING)

    def unit(b, h):
        return rows((2 * b + h) * half, half)

    def zsend(q, b, h, i, k):
        part = X.at[q, unit(b, h), :]
        return send(part, part, z_send.at[q, i], z_recv.at[q, i], zdev(k))

    UP, DOWN = 1, RING - 1
    zc = [[None] * 6 for _ in range(C)]
    for q in range(C):
        with scope("B_wait"):
            for cp in b_copies[q]:
                cp.wait_recv()
        X[q, rows(zi * R, R), :] = dot(p2_ref[...], rb[q]).astype(BF16)
        zc[q][0] = zsend(q, zi, 0, 0, UP)
        zc[q][3] = zsend(q, zi, 1, 3, DOWN)
    for q in range(C):
        with scope("Z0_wait"):
            zc[q][0].wait_recv()
        zc[q][2] = zsend(q, zm, 0, 2, UP)
        with scope("Z3_wait"):
            zc[q][3].wait_recv()
        zc[q][5] = zsend(q, zp, 1, 5, DOWN)
    for q in range(C):
        zc[q][1] = zsend(q, zi, 1, 1, UP)
        zc[q][4] = zsend(q, zi, 0, 4, DOWN)

    with scope("W_wait"):
        for cp in w_copies:
            cp.wait_recv()
        w_loc[0].wait()
        w_loc[1].wait()

    N, F, M, O = range(4)
    pairs = [((zp, 1), (zm, 0)), ((zf, 0), (zf, 1)), ((zp, 0), (zm, 1)), ((zi, 0), (zi, 1))]
    g_copies = [[None] * (RING - 1) for _ in range(4)]
    h_copies = [[None] * (RING - 1) for _ in range(4)]

    def zwait(*which):
        with scope("zwait%d" % which[0]):
            for q in range(C):
                for i in which:
                    zc[q][i].wait_recv()

    def first(i):
        with scope("first%d" % i):
            xs = [jnp.concatenate([X[q, unit(*u), :] for u in pairs[i]], axis=0) for q in range(C)]
            for k in (2, 1, 3, 0):
                dst_x = lax.rem(x + k, RING)
                acc = dot(xs[0], wgu[dst_x, pl.ds(0, DC), :])
                for q in range(1, C):
                    acc = acc + dot(xs[q], wgu[dst_x, pl.ds(q * DC, DC), :])
                if k == 0:
                    own[i] = acc
                else:
                    gp[i, k - 1] = acc.astype(BF16)
                    g_copies[i][k - 1] = send(gp.at[i, k - 1], hr.at[i, k - 1], g_send.at[i, k - 1],
                                              g_recv.at[i, k - 1], xdev(k))

    def second(i):
        with scope("gwait%d" % i):
            for k in range(RING - 1):
                g_copies[i][k].wait_recv()
        with scope("second%d" % i):
            total = own[i]
            for k in range(RING - 1):
                total = total + hr[i, k].astype(F32)
            g = total[:, :inner]
            u = total[:, inner:]
            part = H.at[i, :, cols(x * inner, inner)]
            part[...] = (g / (1.0 + jnp.exp(-g)) * u).astype(BF16)
            for k in (2, 1, 3):
                h_copies[i][k - 1] = send(part, part, h_send.at[i, k - 1], h_recv.at[i, k - 1], xdev(k))

    def hwait(i):
        with scope("hwait%d" % i):
            for k in range(RING - 1):
                h_copies[i][k].wait_recv()

    def dwait(q):
        with scope("dwait%d" % q):
            for cp in d_copies[q]:
                cp.wait_recv()
            w_loc[2 + q].wait()

    def down(i, q):
        return dot(H[i], wd[q])

    rc = [[None] * 6 for _ in range(C)]

    def rsend(buf, into, q, step):
        for j, k in ((0, UP), (1, DOWN)):
            i = step + 3 * j
            rc[q][i] = send(buf.at[q, pl.ds(j * half, half), :], into.at[q, j],
                            r_send.at[q, i], r_recv.at[q, i], zdev(k))

    def near(q):
        with scope("near%d" % q):
            pnear[q] = down(N, q).astype(BF16)

    def far(q):
        with scope("far%d" % q):
            pfar[q] = down(F, q).astype(BF16)
            rsend(pfar, rfar, q, 0)

    def combine(q):
        with scope("comb%d" % q):
            part = down(M, q)
        with scope("S1w%d" % q):
            rc[q][0].wait_recv()
            rc[q][3].wait_recv()
        for j in range(2):
            pcomb[q, pl.ds(j * half, half), :] = (part[j * half:(j + 1) * half] + rfar[q, j].astype(F32)).astype(BF16)
        rsend(pcomb, rcomb, q, 2)

    first(N)
    first(O)
    second(N)
    zwait(2, 5)
    first(F)
    zwait(1, 4)
    first(M)
    hwait(N)
    dwait(0)
    near(0)
    rsend(pnear, rdir, 0, 1)
    second(F)
    d_copies.append(send_down(1))
    second(M)
    second(O)
    hwait(F)
    far(0)
    dwait(1)
    far(1)
    near(1)
    hwait(M)
    combine(0)
    rsend(pnear, rdir, 1, 1)
    combine(1)
    hwait(O)
    with scope("own"):
        for q in range(C):
            pown[q] = down(O, q)

    cc = [[], []]
    for q in range(C):
        with scope("S3w"):
            for i in (1, 4, 2, 5):
                rc[q][i].wait_recv()
        y_lo = pown[q, pl.ds(0, half), :] + rcomb[q, 0].astype(F32) + rdir[q, 1].astype(F32)
        y_hi = pown[q, pl.ds(half, half), :] + rcomb[q, 1].astype(F32) + rdir[q, 0].astype(F32)
        y = jnp.concatenate([y_lo.astype(BF16), y_hi.astype(BF16)], axis=0)
        sr[q] = dot(p2t_ref[...], y).astype(BF16)
        for k in range(1, n_ep):
            dst_e = lax.rem(ep + k, n_ep)
            cc[q].append(send(sr.at[q, rows(dst_e * 16, 16), :], rr.at[q, rows(ep * 16, 16), :],
                              c_send.at[q, k - 1], c_recv.at[q, k - 1], edev(k)))
        rr[q, rows(ep * 16, 16), :] = sr[q, rows(ep * 16, 16), :]
    dc = [[], []]
    for q in range(C):
        with scope("RBw"):
            for cp in cc[q]:
                cp.wait_recv()
        ts[q] = dot(p1t_ref[...], rr[q]).astype(BF16)
        for k in (2, 1, 3):
            dst_x = lax.rem(x + k, RING)
            dc[q].append(send(ts.at[q, rows(dst_x * slots, slots), :], ret_ref.at[:, cols(x * D4 + q * DC, DC)],
                              d_send.at[q, k - 1], d_recv.at[q, k - 1], xdev(k)))
        ret_ref[:, cols(x * D4 + q * DC, DC)] = ts[q, rows(x * slots, slots), :]
    with scope("RAw"):
        for q in range(C):
            for cp in dc[q]:
                cp.wait_recv()
    with scope("sends"):
        for cp in everything:
            cp.wait_send()


def body(tokens, expert_ids, gate_q, w_gate, w_up, w_down):
    n_ep = lax.axis_size("ep")
    T, width = tokens.shape
    D4 = width // RING
    DC = D4 // C
    slots = n_ep * CAP
    R = slots * RING
    inner = w_down.shape[1]
    per = CAP * RING

    p1 = np.zeros((n_ep * 16, R), np.float32)
    p2 = np.zeros((R, n_ep * 16), np.float32)
    for e in range(n_ep):
        for s in range(RING):
            for q in range(CAP):
                p1[e * 16 + s * CAP + q, s * slots + e * CAP + q] = 1
        for j in range(per):
            p2[e * per + j, e * 16 + j] = 1
    consts = [jnp.asarray(m, BF16) for m in (p1, p1.T, p2, p2.T)]

    vm = pl.BlockSpec(memory_space=pltpu.VMEM)
    anyspec = pl.BlockSpec(memory_space=pl.ANY)
    V = pltpu.VMEM
    DMA = pltpu.SemaphoreType.DMA
    half = R // 2
    scratch = [
        V((T, width), BF16),
        V((C, 3, slots, DC), BF16),
        V((C, R, DC), BF16),
        V((C, n_ep * 16, DC), BF16),
        V((C, n_ep * 16, DC), BF16),
        V((C, RING * R, DC), BF16),
        V((RING, D4, 2 * inner), BF16),
        V((C, RING * inner, DC), BF16),
        V((RING, 3, R, 2 * inner), BF16),
        V((RING, R, 2 * inner), F32),
        V((RING, 3, R, 2 * inner), BF16),
        V((RING, R, RING * inner), BF16),
        V((C, R, DC), F32),
        V((C, R, DC), BF16),
        V((C, R, DC), BF16),
        V((C, R, DC), BF16),
        V((C, 2, half, DC), BF16),
        V((C, 2, half, DC), BF16),
        V((C, 2, half, DC), BF16),
        V((C, n_ep * 16, DC), BF16),
        V((C, n_ep * 16, DC), BF16),
        V((C, R, DC), BF16),
        DMA((3 + C,)), DMA((2 + C, 3)), DMA((2 + C, 3)), DMA((C, 3)), DMA((C, 3)),
        DMA((C, n_ep - 1)), DMA((C, n_ep - 1)), DMA((C, 6)), DMA((C, 6)),
        DMA((4, 3)), DMA((4, 3)), DMA((4, 3)), DMA((4, 3)), DMA((C, 6)), DMA((C, 6)),
        DMA((C, n_ep - 1)), DMA((C, n_ep - 1)), DMA((C, 3)), DMA((C, 3)),
    ]
    ret, scal = pl.pallas_call(
        kernel,
        out_shape=(jax.ShapeDtypeStruct((slots, width), BF16), jax.ShapeDtypeStruct((slots, T), F32)),
        in_specs=[vm] * 6 + [anyspec] * 4,
        out_specs=(vm, vm),
        scratch_shapes=scratch,
        compiler_params=pltpu.CompilerParams(collective_id=0, has_side_effects=True, vmem_limit_bytes=60 * 1024 * 1024),
        name="experts",
    )(expert_ids.T, gate_q.T, *consts, tokens, w_gate, w_up, w_down)
    mixed = lax.dot_general(scal, ret.astype(F32), (((0,), (0,)), ((), ())))
    return mixed.astype(BF16)


def solution(mesh):
    in_specs = (
        P(("ep", "etp"), None),
        P(("ep", "etp"), None),
        P(("ep", "etp"), None),
        P("ep", None, "etp"),
        P("ep", None, "etp"),
        P("ep", "etp", None),
    )
    out_specs = P(("ep", "etp"), None)
    return jax.shard_map(body, mesh=mesh, in_specs=in_specs, out_specs=out_specs, check_vma=False)
```

```python
import jax
import jax.numpy as jnp
import numpy as np
from jax import lax
from jax.experimental import pallas as pl
from jax.experimental.pallas import tpu as pltpu
from jax.sharding import PartitionSpec as P

CAP = 3
RING = 4
C = 2
CHUNKS = (4, 4, 3, 3)
MESH = pl.DeviceIdType.MESH
F32 = jnp.float32
BF16 = jnp.bfloat16
scope = jax.named_scope


def third(c):
    return lax.shift_right_logical(c * 43691, 17)


def dot(a, b):
    return jnp.dot(a, b, preferred_element_type=F32)


def kernel(ids_ref, gate_ref, p1_ref, p1t_ref, p2_ref, p2t_ref, tok_hbm, wg_hbm, wu_hbm, wd_hbm,
           ret_ref, scal_ref,
           tok, bs, xa, sb, rb, X, wgu, wd, gp, own, hr, H, pfar, pnear, pcomb, rfar, rdir, rcomb,
           sr, rr, ts,
           loc_sem, w_send, w_recv, a_send, a_recv, b_send, b_recv, z_send, z_recv, g_send, g_recv,
           h_send, h_recv, r_send, r_recv, c_send, c_recv, d_send, d_recv):
    ep = lax.axis_index("ep")
    etp = lax.axis_index("etp")
    n_ep = lax.axis_size("ep")
    zi = etp // RING
    x = etp % RING
    width = tok.shape[1]
    D4 = width // RING
    DC = D4 // C
    slots = n_ep * CAP
    R = slots * RING
    half = R // 2
    inner = wd.shape[0] // RING

    def xdev(k):
        return (ep, zi * RING + lax.rem(x + k, RING))

    def zdev(k):
        return (ep, lax.rem(zi + k, RING) * RING + x)

    def edev(k):
        return (lax.rem(ep + k, n_ep), etp)

    part = D4 // sum(CHUNKS)
    out = []
    for n in CHUNKS:
        out.append((sum(w for _, w in out), n * part))
    Q = len(out)
    others = (n_ep - 1) * 16

    everything = []

    def send(src, dst, ssem, rsem, dev):
        c = pltpu.make_async_remote_copy(src_ref=src, dst_ref=dst, send_sem=ssem, recv_sem=rsem,
                                         device_id=dev, device_id_type=MESH)
        c.start()
        everything.append(c)
        return c

    def send_group(src, dst, ssem, rsem, dev):
        pltpu.make_async_remote_copy(src_ref=src, dst_ref=dst, send_sem=ssem, recv_sem=rsem,
                                     device_id=dev, device_id_type=MESH).start()

    def wait_bytes(ref, sem):
        pltpu.make_async_copy(ref, ref, sem).wait()

    def rows(start, size):
        return pl.ds(pl.multiple_of(start, 16), size)

    def cols(start, size):
        return pl.ds(pl.multiple_of(start, 128), size)

    tok_copy = pltpu.make_async_copy(tok_hbm, tok, loc_sem.at[0])
    tok_copy.start()
    w_loc = [
        pltpu.make_async_copy(wg_hbm.at[0, rows(x * D4, D4), :], wgu.at[x, :, pl.ds(0, inner)], loc_sem.at[1]),
        pltpu.make_async_copy(wu_hbm.at[0, rows(x * D4, D4), :], wgu.at[x, :, pl.ds(inner, inner)], loc_sem.at[2]),
    ] + [
        pltpu.make_async_copy(wd_hbm.at[0, :, cols(x * D4 + o, w)], wd.at[rows(x * inner, inner), pl.ds(o, w)], loc_sem.at[3 + q])
        for q, (o, w) in enumerate(out)
    ]

    barrier = pltpu.get_barrier_semaphore()
    for k in range(1, RING):
        pl.semaphore_signal(barrier, inc=1, device_id=xdev(k), device_id_type=MESH)
    for k in (1, RING - 1):
        pl.semaphore_signal(barrier, inc=1, device_id=zdev(k), device_id_type=MESH)
    for k in range(1, n_ep):
        pl.semaphore_signal(barrier, inc=1, device_id=edev(k), device_id_type=MESH)

    T = tok.shape[0]
    c = lax.broadcasted_iota(jnp.int32, (slots, T), 0)
    expert = third(c)
    slot = (c - CAP * expert).astype(F32)
    hot = jnp.zeros((slots, T), F32)
    weight = jnp.zeros((slots, T), F32)
    for r in range(ids_ref.shape[0]):
        eq = ids_ref[r:r + 1, :] == expert
        hot = jnp.where(eq, 1.0, hot)
        weight = jnp.where(eq, gate_ref[r:r + 1, :].astype(F32), weight)
    before = lax.broadcasted_iota(jnp.int32, (T, T), 0) < lax.broadcasted_iota(jnp.int32, (T, T), 1)
    earlier = dot(hot.astype(BF16), jnp.where(before, 1.0, 0.0).astype(BF16))
    placing = jnp.where(earlier == slot, hot, 0.0)
    scal_ref[...] = (placing * weight * (1.0 / 1024.0)).astype(BF16)
    placing = placing.astype(BF16)

    with scope("tokwait"):
        tok_copy.wait()
    def bucket(q):
        for k in (2, 1, 3, 0):
            piece = dot(placing, tok[:, cols(lax.rem(x + k, RING) * D4 + q * DC, DC)]).astype(BF16)
            if k == 0:
                xa[q, rows(x * slots, slots), :] = piece
            else:
                bs[q, k - 1] = piece

    for q in range(C):
        bucket(q)
    with scope("barrier_in"):
        pl.semaphore_wait(barrier, (RING - 1) + 2 + (n_ep - 1))
    a_copies = [[], []]
    for q in range(C):
        for k in (2, 1, 3):
            a_copies[q].append(send(bs.at[q, k - 1], xa.at[q, rows(x * slots, slots), :],
                                    a_send.at[q, k - 1], a_recv.at[q, k - 1], xdev(k)))

    w_copies = []
    for i, k in enumerate((1, 3, 2)):
        dst_x = lax.rem(x + k, RING)
        w_copies.append(send(wg_hbm.at[0, rows(dst_x * D4, D4), :], wgu.at[x, :, pl.ds(0, inner)],
                             w_send.at[0, i], w_recv.at[0, i], xdev(k)))
        w_copies.append(send(wu_hbm.at[0, rows(dst_x * D4, D4), :], wgu.at[x, :, pl.ds(inner, inner)],
                             w_send.at[1, i], w_recv.at[1, i], xdev(k)))

    def send_down(q):
        o, w = out[q]
        copies = []
        for i, k in enumerate((1, 3, 2)):
            dst_x = lax.rem(x + k, RING)
            copies.append(send(wd_hbm.at[0, :, cols(dst_x * D4 + o, w)],
                               wd.at[rows(x * inner, inner), pl.ds(o, w)],
                               w_send.at[2 + q, i], w_recv.at[2 + q, i], xdev(k)))
        return copies

    d_copies = [send_down(0)]
    for cp in w_loc:
        cp.start()

    for q in range(C):
        with scope("A_wait"):
            for cp in a_copies[q]:
                cp.wait_recv()
        sb[q] = dot(p1_ref[...], xa[q]).astype(BF16)
        for k in range(1, n_ep):
            dst_e = lax.rem(ep + k, n_ep)
            send_group(sb.at[q, rows(dst_e * 16, 16), :], rb.at[q, rows(ep * 16, 16), :],
                       b_send.at[q], b_recv.at[q], edev(k))
        rb[q, rows(ep * 16, 16), :] = sb[q, rows(ep * 16, 16), :]

    zm = lax.rem(zi + RING - 1, RING)
    zp = lax.rem(zi + 1, RING)
    zf = lax.rem(zi + 2, RING)

    def unit(b, h):
        return rows((2 * b + h) * half, half)

    def zsend(q, b, h, i, k):
        part = X.at[q, unit(b, h), :]
        return send(part, part, z_send.at[q, i], z_recv.at[q, i], zdev(k))

    UP, DOWN = 1, RING - 1
    zc = [[None] * 6 for _ in range(C)]
    for q in range(C):
        with scope("B_wait"):
            wait_bytes(rb.at[q, pl.ds(0, others), :], b_recv.at[q])
        X[q, rows(zi * R, R), :] = dot(p2_ref[...], rb[q]).astype(BF16)
        zc[q][0] = zsend(q, zi, 0, 0, UP)
        zc[q][3] = zsend(q, zi, 1, 3, DOWN)
    for q in range(C):
        with scope("Z0_wait"):
            zc[q][0].wait_recv()
        zc[q][2] = zsend(q, zm, 0, 2, UP)
        with scope("Z3_wait"):
            zc[q][3].wait_recv()
        zc[q][5] = zsend(q, zp, 1, 5, DOWN)
    for q in range(C):
        zc[q][1] = zsend(q, zi, 1, 1, UP)
        zc[q][4] = zsend(q, zi, 0, 4, DOWN)

    with scope("W_wait"):
        for cp in w_copies:
            cp.wait_recv()
        w_loc[0].wait()
        w_loc[1].wait()

    N, F, M, O = range(4)
    pairs = [((zp, 1), (zm, 0)), ((zf, 0), (zf, 1)), ((zp, 0), (zm, 1)), ((zi, 0), (zi, 1))]
    g_copies = [[None] * (RING - 1) for _ in range(4)]
    h_copies = [[None] * (RING - 1) for _ in range(4)]

    def zwait(*which):
        with scope("zwait%d" % which[0]):
            for q in range(C):
                for i in which:
                    zc[q][i].wait_recv()

    def first(i):
        with scope("first%d" % i):
            xs = [jnp.concatenate([X[q, unit(*u), :] for u in pairs[i]], axis=0) for q in range(C)]
            for k in (2, 1, 3, 0):
                dst_x = lax.rem(x + k, RING)
                acc = dot(xs[0], wgu[dst_x, pl.ds(0, DC), :])
                for q in range(1, C):
                    acc = acc + dot(xs[q], wgu[dst_x, pl.ds(q * DC, DC), :])
                if k == 0:
                    own[i] = acc
                else:
                    gp[i, k - 1] = acc.astype(BF16)
                    g_copies[i][k - 1] = send(gp.at[i, k - 1], hr.at[i, k - 1], g_send.at[i, k - 1],
                                              g_recv.at[i, k - 1], xdev(k))

    def second(i):
        with scope("gwait%d" % i):
            for k in range(RING - 1):
                g_copies[i][k].wait_recv()
        with scope("second%d" % i):
            total = own[i]
            for k in range(RING - 1):
                total = total + hr[i, k].astype(F32)
            g = total[:, :inner]
            u = total[:, inner:]
            part = H.at[i, :, cols(x * inner, inner)]
            part[...] = (g / (1.0 + jnp.exp(-g)) * u).astype(BF16)
            for k in (2, 1, 3):
                h_copies[i][k - 1] = send(part, part, h_send.at[i, k - 1], h_recv.at[i, k - 1], xdev(k))

    def hwait(i):
        with scope("hwait%d" % i):
            for k in range(RING - 1):
                h_copies[i][k].wait_recv()

    def dwait(q):
        with scope("dwait%d" % q):
            for cp in d_copies[q]:
                cp.wait_recv()
            w_loc[2 + q].wait()

    def down(i, q):
        o, w = out[q]
        return dot(H[i], wd[:, pl.ds(o, w)])

    rc = [[None] * 6 for _ in range(Q)]

    def rsend(buf, into, q, step):
        o, w = out[q]
        for j, k in ((0, UP), (1, DOWN)):
            i = step + 3 * j
            rc[q][i] = send(buf.at[pl.ds(j * half, half), pl.ds(o, w)], into.at[j, :, pl.ds(o, w)],
                            r_send.at[q, i], r_recv.at[q, i], zdev(k))

    def near(q):
        o, w = out[q]
        with scope("near%d" % q):
            pnear[:, pl.ds(o, w)] = down(N, q).astype(BF16)
            rsend(pnear, rdir, q, 1)

    def far(q):
        o, w = out[q]
        with scope("far%d" % q):
            pfar[:, pl.ds(o, w)] = down(F, q).astype(BF16)
            rsend(pfar, rfar, q, 0)

    def combine(q):
        o, w = out[q]
        sl = pl.ds(o, w)
        with scope("comb%d" % q):
            part = down(M, q)
        with scope("S1w%d" % q):
            rc[q][0].wait_recv()
            rc[q][3].wait_recv()
        for j in range(2):
            pcomb[pl.ds(j * half, half), sl] = (part[j * half:(j + 1) * half] + rfar[j, :, sl].astype(F32)).astype(BF16)
        rsend(pcomb, rcomb, q, 2)

    def finish(q):
        o, w = out[q]
        sl = pl.ds(o, w)
        mine = down(O, q)
        with scope("S3w%d" % q):
            for i in (1, 4, 2, 5):
                rc[q][i].wait_recv()
        y_lo = mine[:half] + rcomb[0, :, sl].astype(F32) + rdir[1, :, sl].astype(F32)
        y_hi = mine[half:] + rcomb[1, :, sl].astype(F32) + rdir[0, :, sl].astype(F32)
        y = jnp.concatenate([y_lo.astype(BF16), y_hi.astype(BF16)], axis=0)
        sr[:, sl] = dot(p2t_ref[...], y).astype(BF16)
        for k in range(1, n_ep):
            dst_e = lax.rem(ep + k, n_ep)
            send_group(sr.at[rows(dst_e * 16, 16), sl], rr.at[rows(ep * 16, 16), sl],
                       c_send.at[q], c_recv.at[q], edev(k))
        rr[rows(ep * 16, 16), sl] = sr[rows(ep * 16, 16), sl]

    dc = []

    def give_back(q):
        o, w = out[q]
        sl = pl.ds(o, w)
        with scope("RBw%d" % q):
            wait_bytes(rr.at[pl.ds(0, others), sl], c_recv.at[q])
        ts[:, sl] = dot(p1t_ref[...], rr[:, sl]).astype(BF16)
        for k in (2, 1, 3):
            dst_x = lax.rem(x + k, RING)
            dc.append(send(ts.at[rows(dst_x * slots, slots), sl], ret_ref.at[:, cols(x * D4 + o, w)],
                           d_send.at[q, k - 1], d_recv.at[q, k - 1], xdev(k)))
        ret_ref[:, cols(x * D4 + o, w)] = ts[rows(x * slots, slots), sl]

    first(N)
    zwait(2, 5)
    first(F)
    second(N)
    second(F)
    for q in range(1, Q):
        d_copies.append(send_down(q))
    hwait(N)
    dwait(0)
    near(0)
    hwait(F)
    far(0)
    zwait(1, 4)
    first(M)
    first(O)
    for q in range(1, Q):
        dwait(q)
        near(q)
        far(q)
    second(M)
    second(O)
    hwait(M)
    for q in range(Q):
        combine(q)
    hwait(O)
    finish(0)
    finish(1)
    for q in range(2, Q):
        give_back(q - 2)
        finish(q)
    give_back(Q - 2)
    give_back(Q - 1)
    with scope("RAw"):
        for cp in dc:
            cp.wait_recv()
    with scope("sends"):
        for cp in everything:
            cp.wait_send()
        for q in range(C):
            wait_bytes(sb.at[q, pl.ds(0, others), :], b_send.at[q])
        for q, (o, w) in enumerate(out):
            wait_bytes(sr.at[pl.ds(0, others), pl.ds(o, w)], c_send.at[q])


def body(tokens, expert_ids, gate_q, w_gate, w_up, w_down):
    n_ep = lax.axis_size("ep")
    T, width = tokens.shape
    D4 = width // RING
    DC = D4 // C
    slots = n_ep * CAP
    R = slots * RING
    inner = w_down.shape[1]
    per = CAP * RING

    p1 = np.zeros((n_ep * 16, R), np.float32)
    p2 = np.zeros((R, n_ep * 16), np.float32)
    for e in range(n_ep):
        for s in range(RING):
            for q in range(CAP):
                p1[e * 16 + s * CAP + q, s * slots + e * CAP + q] = 1
        for j in range(per):
            p2[e * per + j, e * 16 + j] = 1
    consts = [jnp.asarray(m, BF16) for m in (p1, p1.T, p2, p2.T)]

    vm = pl.BlockSpec(memory_space=pltpu.VMEM)
    anyspec = pl.BlockSpec(memory_space=pl.ANY)
    V = pltpu.VMEM
    DMA = pltpu.SemaphoreType.DMA
    half = R // 2
    Q = len(CHUNKS)
    scratch = [
        V((T, width), BF16),
        V((C, 3, slots, DC), BF16),
        V((C, R, DC), BF16),
        V((C, n_ep * 16, DC), BF16),
        V((C, n_ep * 16, DC), BF16),
        V((C, RING * R, DC), BF16),
        V((RING, D4, 2 * inner), BF16),
        V((RING * inner, D4), BF16),
        V((RING, 3, R, 2 * inner), BF16),
        V((RING, R, 2 * inner), F32),
        V((RING, 3, R, 2 * inner), BF16),
        V((RING, R, RING * inner), BF16),
        V((R, D4), BF16),
        V((R, D4), BF16),
        V((R, D4), BF16),
        V((2, half, D4), BF16),
        V((2, half, D4), BF16),
        V((2, half, D4), BF16),
        V((n_ep * 16, D4), BF16),
        V((n_ep * 16, D4), BF16),
        V((R, D4), BF16),
        DMA((3 + Q,)), DMA((2 + Q, 3)), DMA((2 + Q, 3)), DMA((C, 3)), DMA((C, 3)),
        DMA((C,)), DMA((C,)), DMA((C, 6)), DMA((C, 6)),
        DMA((4, 3)), DMA((4, 3)), DMA((4, 3)), DMA((4, 3)), DMA((Q, 6)), DMA((Q, 6)),
        DMA((Q,)), DMA((Q,)), DMA((Q, 3)), DMA((Q, 3)),
    ]
    ret, scal = pl.pallas_call(
        kernel,
        out_shape=(jax.ShapeDtypeStruct((slots, width), BF16), jax.ShapeDtypeStruct((slots, T), BF16)),
        in_specs=[vm] * 6 + [anyspec] * 4,
        out_specs=(vm, vm),
        scratch_shapes=scratch,
        compiler_params=pltpu.CompilerParams(collective_id=0, has_side_effects=True, vmem_limit_bytes=60 * 1024 * 1024),
        name="experts",
    )(expert_ids.T, gate_q.T, *consts, tokens, w_gate, w_up, w_down)
    mixed = lax.dot_general(scal, ret, (((0,), (0,)), ((), ())), preferred_element_type=F32)
    return mixed.astype(BF16)


def solution(mesh):
    in_specs = (
        P(("ep", "etp"), None),
        P(("ep", "etp"), None),
        P(("ep", "etp"), None),
        P("ep", None, "etp"),
        P("ep", None, "etp"),
        P("ep", "etp", None),
    )
    out_specs = P(("ep", "etp"), None)
    return jax.shard_map(body, mesh=mesh, in_specs=in_specs, out_specs=out_specs, check_vma=False)
```

```python
import jax
import jax.numpy as jnp
import numpy as np
from jax import lax
from jax.experimental import pallas as pl
from jax.experimental.pallas import tpu as pltpu
from jax.sharding import PartitionSpec as P

CAP = 3
RING = 4
CIN = (3, 4, 4, 3)
CHUNKS = (3, 4, 4, 3)
MESH = pl.DeviceIdType.MESH
F32 = jnp.float32
BF16 = jnp.bfloat16
scope = jax.named_scope


def third(c):
    return lax.shift_right_logical(c * 43691, 17)


def dot(a, b):
    return jnp.dot(a, b, preferred_element_type=F32)


def kernel(ids_ref, gate_ref, p1_ref, p1t_ref, p2_ref, p2t_ref, tok_hbm, wg_hbm, wu_hbm, wd_hbm,
           ret_ref, scal_ref,
           tok, bs, xa, sb, rb, X, wgu, wd, gp, own, hr, H, pfar, pnear, pcomb, rfar, rdir, rcomb,
           sr, rr, ts,
           loc_sem, send_sem, w_recv, wd_recv, a_recv, b_recv, zn_recv, zf_recv, zm_recv, g_recv,
           h_recv, rf_recv, ro_recv, c_recv, d_recv):
    ep = lax.axis_index("ep")
    etp = lax.axis_index("etp")
    n_ep = lax.axis_size("ep")
    zi = etp // RING
    x = etp % RING
    width = tok.shape[1]
    D4 = width // RING
    slots = n_ep * CAP
    R = slots * RING
    half = R // 2
    inner = wd.shape[0] // RING

    def xdev(k):
        return (ep, zi * RING + lax.rem(x + k, RING))

    def zdev(k):
        return (ep, lax.rem(zi + k, RING) * RING + x)

    def edev(k):
        return (lax.rem(ep + k, n_ep), etp)

    def spans(parts):
        made = []
        for n in parts:
            made.append((sum(w for _, w in made), n * D4 // sum(parts)))
        return made

    into, out = spans(CIN), spans(CHUNKS)
    C, Q = len(into), len(out)
    others = (n_ep - 1) * 16

    A_S, W_S, D_S, B_S, Z_S, G_S, H_S, R_S, C_S, E_S = range(10)

    def send(src, dst, group, rsem, dev):
        pltpu.make_async_remote_copy(src_ref=src, dst_ref=dst, send_sem=send_sem.at[group], recv_sem=rsem,
                                     device_id=dev, device_id_type=MESH).start()

    def wait_bytes(ref, sem):
        pltpu.make_async_copy(ref, ref, sem).wait()

    def rows(start, size):
        return pl.ds(pl.multiple_of(start, 16), size)

    def cols(start, size):
        return pl.ds(pl.multiple_of(start, 128), size)

    tok_copy = pltpu.make_async_copy(tok_hbm, tok, loc_sem.at[0])
    tok_copy.start()
    w_loc = [
        pltpu.make_async_copy(wg_hbm.at[0, rows(x * D4, D4), :], wgu.at[x, :, pl.ds(0, inner)], loc_sem.at[1]),
        pltpu.make_async_copy(wu_hbm.at[0, rows(x * D4, D4), :], wgu.at[x, :, pl.ds(inner, inner)], loc_sem.at[2]),
    ] + [
        pltpu.make_async_copy(wd_hbm.at[0, :, cols(x * D4 + o, w)], wd.at[rows(x * inner, inner), pl.ds(o, w)], loc_sem.at[3 + q])
        for q, (o, w) in enumerate(out)
    ]

    barrier = pltpu.get_barrier_semaphore()
    for k in range(1, RING):
        pl.semaphore_signal(barrier, inc=1, device_id=xdev(k), device_id_type=MESH)
    for k in (1, RING - 1):
        pl.semaphore_signal(barrier, inc=1, device_id=zdev(k), device_id_type=MESH)
    for k in range(1, n_ep):
        pl.semaphore_signal(barrier, inc=1, device_id=edev(k), device_id_type=MESH)

    T = tok.shape[0]
    c = lax.broadcasted_iota(jnp.int32, (slots, T), 0)
    expert = third(c)
    slot = (c - CAP * expert).astype(F32)
    hot = jnp.zeros((slots, T), F32)
    weight = jnp.zeros((slots, T), F32)
    for r in range(ids_ref.shape[0]):
        eq = ids_ref[r:r + 1, :] == expert
        hot = jnp.where(eq, 1.0, hot)
        weight = jnp.where(eq, gate_ref[r:r + 1, :].astype(F32), weight)
    before = lax.broadcasted_iota(jnp.int32, (T, T), 0) < lax.broadcasted_iota(jnp.int32, (T, T), 1)
    earlier = dot(hot.astype(BF16), jnp.where(before, 1.0, 0.0).astype(BF16))
    placing = jnp.where(earlier == slot, hot, 0.0)
    scal_ref[...] = (placing * weight * (1.0 / 1024.0)).astype(BF16)
    placing = placing.astype(BF16)

    with scope("tokwait"):
        tok_copy.wait()
    def bucket(q):
        o, w = into[q]
        for k in (2, 1, 3, 0):
            piece = dot(placing, tok[:, cols(lax.rem(x + k, RING) * D4 + o, w)]).astype(BF16)
            if k == 0:
                xa[rows(x * slots, slots), pl.ds(o, w)] = piece
            else:
                bs[k - 1, :, pl.ds(o, w)] = piece

    for q in range(C):
        bucket(q)
    with scope("barrier_in"):
        pl.semaphore_wait(barrier, (RING - 1) + 2 + (n_ep - 1))
    for q, (o, w) in enumerate(into):
        for k in (2, 1, 3):
            send(bs.at[k - 1, :, pl.ds(o, w)], xa.at[rows(x * slots, slots), pl.ds(o, w)],
                 A_S, a_recv.at[q], xdev(k))

    for k in (1, 3, 2):
        dst_x = lax.rem(x + k, RING)
        send(wg_hbm.at[0, rows(dst_x * D4, D4), :], wgu.at[x, :, pl.ds(0, inner)], W_S, w_recv, xdev(k))
        send(wu_hbm.at[0, rows(dst_x * D4, D4), :], wgu.at[x, :, pl.ds(inner, inner)], W_S, w_recv, xdev(k))

    def send_down(q):
        o, w = out[q]
        for k in (1, 3, 2):
            dst_x = lax.rem(x + k, RING)
            send(wd_hbm.at[0, :, cols(dst_x * D4 + o, w)], wd.at[rows(x * inner, inner), pl.ds(o, w)],
                 D_S, wd_recv.at[q], xdev(k))

    send_down(0)
    for cp in w_loc:
        cp.start()

    for q, (o, w) in enumerate(into):
        sl = pl.ds(o, w)
        with scope("A_wait"):
            wait_bytes(xa.at[pl.ds(0, (RING - 1) * slots), sl], a_recv.at[q])
        sb[:, sl] = dot(p1_ref[...], xa[:, sl]).astype(BF16)
        for k in range(1, n_ep):
            dst_e = lax.rem(ep + k, n_ep)
            send(sb.at[rows(dst_e * 16, 16), sl], rb.at[rows(ep * 16, 16), sl], B_S, b_recv.at[q], edev(k))
        rb[rows(ep * 16, 16), sl] = sb[rows(ep * 16, 16), sl]

    zm = lax.rem(zi + RING - 1, RING)
    zp = lax.rem(zi + 1, RING)
    zf = lax.rem(zi + 2, RING)

    def unit(b, h):
        return rows((2 * b + h) * half, half)

    def zsend(q, b, h, rsem, k):
        part = X.at[unit(b, h), pl.ds(*into[q])]
        send(part, part, Z_S, rsem, zdev(k))

    def zwait(sem, q, count):
        wait_bytes(X.at[pl.ds(0, count * half), pl.ds(*into[q])], sem)

    UP, DOWN = 1, RING - 1

    def outset(q):
        sl = pl.ds(*into[q])
        with scope("B_wait"):
            wait_bytes(rb.at[pl.ds(0, others), sl], b_recv.at[q])
        X[rows(zi * R, R), sl] = dot(p2_ref[...], rb[:, sl]).astype(BF16)
        zsend(q, zi, 0, zn_recv.at[q, 0], UP)
        zsend(q, zi, 1, zn_recv.at[q, 1], DOWN)

    def forward(q):
        with scope("Z0_wait"):
            zwait(zn_recv.at[q, 0], q, 1)
        zsend(q, zm, 0, zf_recv.at[q], UP)
        with scope("Z3_wait"):
            zwait(zn_recv.at[q, 1], q, 1)
        zsend(q, zp, 1, zf_recv.at[q], DOWN)

    for q in range(C):
        outset(q)
    for q in range(C):
        forward(q)
    for q in range(C):
        zsend(q, zi, 1, zm_recv.at[q], UP)
        zsend(q, zi, 0, zm_recv.at[q], DOWN)

    with scope("W_wait"):
        wait_bytes(wgu.at[pl.ds(0, RING - 1)], w_recv)
        w_loc[0].wait()
        w_loc[1].wait()

    N, F, M, O = range(4)
    pairs = [((zp, 1), (zm, 0)), ((zf, 0), (zf, 1)), ((zp, 0), (zm, 1)), ((zi, 0), (zi, 1))]
    def first(i):
        with scope("first%d" % i):
            xs = jnp.concatenate([X[unit(*u), :] for u in pairs[i]], axis=0)
            for k in (2, 1, 3, 0):
                dst_x = lax.rem(x + k, RING)
                acc = dot(xs, wgu[dst_x])
                if k == 0:
                    own[i] = acc
                else:
                    gp[i, k - 1] = acc.astype(BF16)
                    send(gp.at[i, k - 1], hr.at[i, k - 1], G_S, g_recv.at[i], xdev(k))

    def second(i):
        with scope("gwait%d" % i):
            wait_bytes(hr.at[i], g_recv.at[i])
        with scope("second%d" % i):
            total = own[i]
            for k in range(RING - 1):
                total = total + hr[i, k].astype(F32)
            g = total[:, :inner]
            u = total[:, inner:]
            part = H.at[i, :, cols(x * inner, inner)]
            part[...] = (g / (1.0 + jnp.exp(-g)) * u).astype(BF16)
            for k in (2, 1, 3):
                send(part, part, H_S, h_recv.at[i], xdev(k))

    def hwait(i):
        with scope("hwait%d" % i):
            wait_bytes(H.at[i, :, pl.ds(0, (RING - 1) * inner)], h_recv.at[i])

    def dwait(q):
        with scope("dwait%d" % q):
            wait_bytes(wd.at[pl.ds(0, (RING - 1) * inner), pl.ds(*out[q])], wd_recv.at[q])
            w_loc[2 + q].wait()

    def down(i, q):
        o, w = out[q]
        return dot(H[i], wd[:, pl.ds(o, w)])

    def rsend(buf, into, q, rsem):
        o, w = out[q]
        for j, k in ((0, UP), (1, DOWN)):
            send(buf.at[pl.ds(j * half, half), pl.ds(o, w)], into.at[j, :, pl.ds(o, w)], R_S, rsem, zdev(k))

    def near(q):
        o, w = out[q]
        with scope("near%d" % q):
            pnear[:, pl.ds(o, w)] = down(N, q).astype(BF16)
            rsend(pnear, rdir, q, ro_recv.at[q])

    def far(q):
        o, w = out[q]
        with scope("far%d" % q):
            pfar[:, pl.ds(o, w)] = down(F, q).astype(BF16)
            rsend(pfar, rfar, q, rf_recv.at[q])

    def combine(q):
        o, w = out[q]
        sl = pl.ds(o, w)
        with scope("comb%d" % q):
            part = down(M, q)
        with scope("S1w%d" % q):
            wait_bytes(X.at[pl.ds(0, 2 * half), sl], rf_recv.at[q])
        for j in range(2):
            pcomb[pl.ds(j * half, half), sl] = (part[j * half:(j + 1) * half] + rfar[j, :, sl].astype(F32)).astype(BF16)
        rsend(pcomb, rcomb, q, ro_recv.at[q])

    def finish(q):
        o, w = out[q]
        sl = pl.ds(o, w)
        mine = down(O, q)
        with scope("S3w%d" % q):
            wait_bytes(X.at[pl.ds(0, 4 * half), sl], ro_recv.at[q])
        y_lo = mine[:half] + rcomb[0, :, sl].astype(F32) + rdir[1, :, sl].astype(F32)
        y_hi = mine[half:] + rcomb[1, :, sl].astype(F32) + rdir[0, :, sl].astype(F32)
        y = jnp.concatenate([y_lo.astype(BF16), y_hi.astype(BF16)], axis=0)
        sr[:, sl] = dot(p2t_ref[...], y).astype(BF16)
        for k in range(1, n_ep):
            dst_e = lax.rem(ep + k, n_ep)
            send(sr.at[rows(dst_e * 16, 16), sl], rr.at[rows(ep * 16, 16), sl], C_S, c_recv.at[q], edev(k))
        rr[rows(ep * 16, 16), sl] = sr[rows(ep * 16, 16), sl]

    def give_back(q):
        o, w = out[q]
        sl = pl.ds(o, w)
        with scope("RBw%d" % q):
            wait_bytes(rr.at[pl.ds(0, others), sl], c_recv.at[q])
        ts[:, sl] = dot(p1t_ref[...], rr[:, sl]).astype(BF16)
        for k in (2, 1, 3):
            dst_x = lax.rem(x + k, RING)
            send(ts.at[rows(dst_x * slots, slots), sl], ret_ref.at[:, cols(x * D4 + o, w)], E_S, d_recv, xdev(k))
        ret_ref[:, cols(x * D4 + o, w)] = ts[rows(x * slots, slots), sl]

    first(N)
    with scope("zfwait"):
        for q in range(C):
            zwait(zf_recv.at[q], q, 2)
    first(F)
    second(N)
    second(F)
    send_down(1)
    send_down(2)
    hwait(N)
    dwait(0)
    near(0)
    hwait(F)
    far(0)
    with scope("zmwait"):
        for q in range(C):
            zwait(zm_recv.at[q], q, 2)
    first(M)
    send_down(3)
    for q in (1, 2):
        dwait(q)
        near(q)
        far(q)
    second(M)
    first(O)
    dwait(3)
    near(3)
    far(3)
    second(O)
    hwait(M)
    for q in range(Q):
        combine(q)
    hwait(O)
    finish(0)
    finish(1)
    for q in range(2, Q):
        give_back(q - 2)
        finish(q)
    give_back(Q - 2)
    give_back(Q - 1)
    with scope("RAw"):
        wait_bytes(ts.at[pl.ds(0, (RING - 1) * slots), :], d_recv)
    with scope("sends"):
        for group, ref in ((A_S, bs), (W_S, wgu.at[pl.ds(0, RING - 1)]),
                           (D_S, wd.at[pl.ds(0, (RING - 1) * inner), :]),
                           (B_S, sb.at[pl.ds(0, others), :]), (Z_S, X.at[pl.ds(0, 6 * half), :]),
                           (G_S, hr), (H_S, H.at[:, :, pl.ds(0, (RING - 1) * inner)]),
                           (R_S, X.at[pl.ds(0, 6 * half), :]), (C_S, sr.at[pl.ds(0, others), :]),
                           (E_S, ts.at[pl.ds(0, (RING - 1) * slots), :])):
            wait_bytes(ref, send_sem.at[group])


def body(tokens, expert_ids, gate_q, w_gate, w_up, w_down):
    n_ep = lax.axis_size("ep")
    T, width = tokens.shape
    D4 = width // RING
    slots = n_ep * CAP
    R = slots * RING
    inner = w_down.shape[1]
    per = CAP * RING

    p1 = np.zeros((n_ep * 16, R), np.float32)
    p2 = np.zeros((R, n_ep * 16), np.float32)
    for e in range(n_ep):
        for s in range(RING):
            for q in range(CAP):
                p1[e * 16 + s * CAP + q, s * slots + e * CAP + q] = 1
        for j in range(per):
            p2[e * per + j, e * 16 + j] = 1
    consts = [jnp.asarray(m, BF16) for m in (p1, p1.T, p2, p2.T)]

    vm = pl.BlockSpec(memory_space=pltpu.VMEM)
    anyspec = pl.BlockSpec(memory_space=pl.ANY)
    V = pltpu.VMEM
    DMA = pltpu.SemaphoreType.DMA
    half = R // 2
    C, Q = len(CIN), len(CHUNKS)
    scratch = [
        V((T, width), BF16),
        V((3, slots, D4), BF16),
        V((R, D4), BF16),
        V((n_ep * 16, D4), BF16),
        V((n_ep * 16, D4), BF16),
        V((RING * R, D4), BF16),
        V((RING, D4, 2 * inner), BF16),
        V((RING * inner, D4), BF16),
        V((RING, 3, R, 2 * inner), BF16),
        V((RING, R, 2 * inner), F32),
        V((RING, 3, R, 2 * inner), BF16),
        V((RING, R, RING * inner), BF16),
        V((R, D4), BF16),
        V((R, D4), BF16),
        V((R, D4), BF16),
        V((2, half, D4), BF16),
        V((2, half, D4), BF16),
        V((2, half, D4), BF16),
        V((n_ep * 16, D4), BF16),
        V((n_ep * 16, D4), BF16),
        V((R, D4), BF16),
        DMA((3 + Q,)), DMA((10,)), DMA(()), DMA((Q,)), DMA((C,)), DMA((C,)), DMA((C, 2)), DMA((C,)), DMA((C,)),
        DMA((4,)), DMA((4,)), DMA((Q,)), DMA((Q,)), DMA((Q,)), DMA(()),
    ]
    ret, scal = pl.pallas_call(
        kernel,
        out_shape=(pltpu.VMEM((slots, width), BF16), pltpu.VMEM((slots, T), BF16)),
        in_specs=[vm] * 6 + [anyspec] * 4,
        out_specs=(vm, vm),
        scratch_shapes=scratch,
        compiler_params=pltpu.CompilerParams(collective_id=0, has_side_effects=True, vmem_limit_bytes=60 * 1024 * 1024),
        name="experts",
    )(expert_ids.T, gate_q.T, *consts, tokens, w_gate, w_up, w_down)
    mixed = lax.dot_general(scal, ret, (((0,), (0,)), ((), ())), preferred_element_type=F32)
    return mixed.astype(BF16)


def solution(mesh):
    in_specs = (
        P(("ep", "etp"), None),
        P(("ep", "etp"), None),
        P(("ep", "etp"), None),
        P("ep", None, "etp"),
        P("ep", None, "etp"),
        P("ep", "etp", None),
    )
    out_specs = P(("ep", "etp"), None)
    return jax.shard_map(body, mesh=mesh, in_specs=in_specs, out_specs=out_specs, check_vma=False)
```

```python
import jax
import jax.numpy as jnp
import numpy as np
from jax import lax
from jax.experimental import pallas as pl
from jax.experimental.pallas import tpu as pltpu
from jax.sharding import PartitionSpec as P

CAP = 3
RING = 4
CIN = (4, 4, 4, 2)
CHUNKS = (4, 4, 4, 2)
MESH = pl.DeviceIdType.MESH
F32 = jnp.float32
BF16 = jnp.bfloat16
scope = jax.named_scope


def third(c):
    return lax.shift_right_logical(c * 43691, 17)


def dot(a, b):
    return jnp.dot(a, b, preferred_element_type=F32)


def packed(width):
    return width * 3 // 4 if width % 512 == 0 else width


def pack(p, src):
    w = src.shape[1]
    keep = packed(w)
    made = dot(p[0], src[:, :keep])
    if keep < w:
        made = made + jnp.concatenate([dot(p[1 + j], src[:, keep:]) for j in range(3)], axis=1)
    return made.astype(BF16)


def unpack(p, src, w):
    keep = packed(w)
    made = dot(p[0], src).astype(BF16)
    if keep < w:
        part = w - keep
        rest = dot(p[1], src[:, :part]) + dot(p[2], src[:, part:2 * part]) + dot(p[3], src[:, 2 * part:])
        made = jnp.concatenate([made, rest.astype(BF16)], axis=1)
    return made


def kernel(ids_hbm, gate_hbm, p1_hbm, p1t_hbm, p2_hbm, p2t_hbm, tok_hbm, wg_hbm, wu_hbm, wd_hbm,
           ret_ref, scal_ref,
           ids_ref, gate_ref, p1_ref, p1t_ref, p2_ref, p2t_ref, tok, bs, xa, sb, rb, X, wgu, wd, gp, own, hr, H, pfar, pnear, pcomb, rfar, rdir, rcomb,
           sr, rr, ts,
           loc_sem, send_sem, w_recv, wd_recv, a_recv, b_recv, zn_recv, zf_recv, zm_recv, g_recv,
           h_recv, rf_recv, ro_recv, c_recv, d_recv):
    ep = lax.axis_index("ep")
    etp = lax.axis_index("etp")
    n_ep = lax.axis_size("ep")
    zi = etp // RING
    x = etp % RING
    width = tok.shape[1]
    D4 = width // RING
    slots = n_ep * CAP
    R = slots * RING
    half = R // 2
    inner = wd.shape[0] // RING

    def xdev(k):
        return (ep, zi * RING + lax.rem(x + k, RING))

    def zdev(k):
        return (ep, lax.rem(zi + k, RING) * RING + x)

    def edev(k):
        return (lax.rem(ep + k, n_ep), etp)

    def spans(parts):
        made = []
        for n in parts:
            made.append((sum(w for _, w in made), n * D4 // sum(parts)))
        return made

    into, out = spans(CIN), spans(CHUNKS)
    C, Q = len(into), len(out)
    others = (n_ep - 1) * 16

    A_S, W_S, D_S, B_S, Z_S, G_S, H_S, R_S, C_S, E_S = range(10)

    def send(src, dst, group, rsem, dev):
        pltpu.make_async_remote_copy(src_ref=src, dst_ref=dst, send_sem=send_sem.at[group], recv_sem=rsem,
                                     device_id=dev, device_id_type=MESH).start()

    def wait_bytes(ref, sem):
        pltpu.make_async_copy(ref, ref, sem).wait()

    def rows(start, size):
        return pl.ds(pl.multiple_of(start, 16), size)

    def cols(start, size):
        return pl.ds(pl.multiple_of(start, 128), size)

    barrier = pltpu.get_barrier_semaphore()
    for k in range(1, RING):
        pl.semaphore_signal(barrier, inc=1, device_id=xdev(k), device_id_type=MESH)
    for k in (1, RING - 1):
        pl.semaphore_signal(barrier, inc=1, device_id=zdev(k), device_id_type=MESH)
    for k in range(1, n_ep):
        pl.semaphore_signal(barrier, inc=1, device_id=edev(k), device_id_type=MESH)

    ids_copies = [pltpu.make_async_copy(ids_hbm, ids_ref, loc_sem.at[0]),
                  pltpu.make_async_copy(gate_hbm, gate_ref, loc_sem.at[1])]
    tok_copy = pltpu.make_async_copy(tok_hbm, tok, loc_sem.at[2])
    p_copies = [pltpu.make_async_copy(src, dst, loc_sem.at[3 + i])
                for i, (src, dst) in enumerate(((p1_hbm, p1_ref), (p1t_hbm, p1t_ref), (p2_hbm, p2_ref), (p2t_hbm, p2t_ref)))]
    for cp in ids_copies + [tok_copy] + p_copies:
        cp.start()
    w_loc = [
        pltpu.make_async_copy(wg_hbm.at[0, rows(x * D4, D4), :], wgu.at[x, :, pl.ds(0, inner)], loc_sem.at[7]),
        pltpu.make_async_copy(wu_hbm.at[0, rows(x * D4, D4), :], wgu.at[x, :, pl.ds(inner, inner)], loc_sem.at[8]),
    ] + [
        pltpu.make_async_copy(wd_hbm.at[0, :, cols(x * D4 + o, w)], wd.at[rows(x * inner, inner), pl.ds(o, w)], loc_sem.at[9 + q])
        for q, (o, w) in enumerate(out)
    ]

    with scope("idswait"):
        for cp in ids_copies:
            cp.wait()

    T = tok.shape[0]
    c = lax.broadcasted_iota(jnp.int32, (slots, T), 0)
    expert = third(c)
    slot = (c - CAP * expert).astype(F32)
    hot = jnp.zeros((slots, T), F32)
    weight = jnp.zeros((slots, T), F32)
    for r in range(ids_ref.shape[0]):
        eq = ids_ref[r:r + 1, :] == expert
        hot = jnp.where(eq, 1.0, hot)
        weight = jnp.where(eq, gate_ref[r:r + 1, :].astype(F32), weight)
    before = lax.broadcasted_iota(jnp.int32, (T, T), 0) < lax.broadcasted_iota(jnp.int32, (T, T), 1)
    earlier = dot(hot.astype(BF16), jnp.where(before, 1.0, 0.0).astype(BF16))
    placing = jnp.where(earlier == slot, hot, 0.0)
    scal_ref[...] = (placing * weight * (1.0 / 1024.0)).astype(BF16)
    placing = placing.astype(BF16)

    with scope("tokwait"):
        tok_copy.wait()
    def bucket(q):
        o, w = into[q]
        for k in (2, 1, 3, 0):
            piece = dot(placing, tok[:, cols(lax.rem(x + k, RING) * D4 + o, w)]).astype(BF16)
            if k == 0:
                xa[rows(x * slots, slots), pl.ds(o, w)] = piece
            else:
                bs[k - 1, :, pl.ds(o, w)] = piece

    for q in range(C):
        bucket(q)
    with scope("barrier_in"):
        pl.semaphore_wait(barrier, (RING - 1) + 2 + (n_ep - 1))
    for q, (o, w) in enumerate(into):
        for k in (2, 1, 3):
            send(bs.at[k - 1, :, pl.ds(o, w)], xa.at[rows(x * slots, slots), pl.ds(o, w)],
                 A_S, a_recv.at[q], xdev(k))

    for k in (1, 3, 2):
        dst_x = lax.rem(x + k, RING)
        send(wg_hbm.at[0, rows(dst_x * D4, D4), :], wgu.at[x, :, pl.ds(0, inner)], W_S, w_recv, xdev(k))
        send(wu_hbm.at[0, rows(dst_x * D4, D4), :], wgu.at[x, :, pl.ds(inner, inner)], W_S, w_recv, xdev(k))

    def send_down(q):
        o, w = out[q]
        for k in (1, 3, 2):
            dst_x = lax.rem(x + k, RING)
            send(wd_hbm.at[0, :, cols(dst_x * D4 + o, w)], wd.at[rows(x * inner, inner), pl.ds(o, w)],
                 D_S, wd_recv.at[q], xdev(k))

    send_down(0)
    for cp in w_loc:
        cp.start()

    for cp in p_copies:
        cp.wait()

    for q, (o, w) in enumerate(into):
        sl = pl.ds(o, w)
        sp = pl.ds(o, packed(w))
        with scope("A_wait"):
            wait_bytes(xa.at[pl.ds(0, (RING - 1) * slots), sl], a_recv.at[q])
        sb[:, sp] = pack(p1_ref, xa[:, sl])
        for k in range(1, n_ep):
            dst_e = lax.rem(ep + k, n_ep)
            send(sb.at[rows(dst_e * 16, 16), sp], rb.at[rows(ep * 16, 16), sp], B_S, b_recv.at[q], edev(k))
        rb[rows(ep * 16, 16), sp] = sb[rows(ep * 16, 16), sp]

    zm = lax.rem(zi + RING - 1, RING)
    zp = lax.rem(zi + 1, RING)
    zf = lax.rem(zi + 2, RING)

    def unit(b, h):
        return rows((2 * b + h) * half, half)

    def zsend(q, b, h, rsem, k):
        part = X.at[unit(b, h), pl.ds(*into[q])]
        send(part, part, Z_S, rsem, zdev(k))

    def zwait(sem, q, count):
        wait_bytes(X.at[pl.ds(0, count * half), pl.ds(*into[q])], sem)

    UP, DOWN = 1, RING - 1

    def outset(q):
        o, w = into[q]
        sp = pl.ds(o, packed(w))
        with scope("B_wait"):
            wait_bytes(rb.at[pl.ds(0, others), sp], b_recv.at[q])
        X[rows(zi * R, R), pl.ds(o, w)] = unpack(p2_ref, rb[:, sp], w)
        zsend(q, zi, 0, zn_recv.at[q, 0], UP)
        zsend(q, zi, 1, zn_recv.at[q, 1], DOWN)

    def forward(q):
        with scope("Z0_wait"):
            zwait(zn_recv.at[q, 0], q, 1)
        zsend(q, zm, 0, zf_recv.at[q], UP)
        with scope("Z3_wait"):
            zwait(zn_recv.at[q, 1], q, 1)
        zsend(q, zp, 1, zf_recv.at[q], DOWN)

    for q in range(C):
        outset(q)
    for q in range(C):
        forward(q)
    for q in range(C):
        zsend(q, zi, 1, zm_recv.at[q], UP)
        zsend(q, zi, 0, zm_recv.at[q], DOWN)

    with scope("W_wait"):
        wait_bytes(wgu.at[pl.ds(0, RING - 1)], w_recv)
        w_loc[0].wait()
        w_loc[1].wait()

    N, F, M, O = range(4)
    pairs = [((zp, 1), (zm, 0)), ((zf, 0), (zf, 1)), ((zp, 0), (zm, 1)), ((zi, 0), (zi, 1))]
    def first(i):
        with scope("first%d" % i):
            xs = jnp.concatenate([X[unit(*u), :] for u in pairs[i]], axis=0)
            for k in (2, 1, 3, 0):
                dst_x = lax.rem(x + k, RING)
                acc = dot(xs, wgu[dst_x])
                if k == 0:
                    own[i] = acc
                else:
                    gp[i, k - 1] = acc.astype(BF16)
                    send(gp.at[i, k - 1], hr.at[i, k - 1], G_S, g_recv.at[i], xdev(k))

    def second(i):
        with scope("gwait%d" % i):
            wait_bytes(hr.at[i], g_recv.at[i])
        with scope("second%d" % i):
            total = own[i]
            for k in range(RING - 1):
                total = total + hr[i, k].astype(F32)
            g = total[:, :inner]
            u = total[:, inner:]
            part = H.at[i, :, cols(x * inner, inner)]
            part[...] = (g / (1.0 + jnp.exp(-g)) * u).astype(BF16)
            for k in (2, 1, 3):
                send(part, part, H_S, h_recv.at[i], xdev(k))

    def hwait(i):
        with scope("hwait%d" % i):
            wait_bytes(H.at[i, :, pl.ds(0, (RING - 1) * inner)], h_recv.at[i])

    def dwait(q):
        with scope("dwait%d" % q):
            wait_bytes(wd.at[pl.ds(0, (RING - 1) * inner), pl.ds(*out[q])], wd_recv.at[q])
            w_loc[2 + q].wait()

    def down(i, q):
        o, w = out[q]
        return dot(H[i], wd[:, pl.ds(o, w)])

    def rsend(buf, into, q, rsem):
        o, w = out[q]
        for j, k in ((0, UP), (1, DOWN)):
            send(buf.at[pl.ds(j * half, half), pl.ds(o, w)], into.at[j, :, pl.ds(o, w)], R_S, rsem, zdev(k))

    def near(q):
        o, w = out[q]
        with scope("near%d" % q):
            pnear[:, pl.ds(o, w)] = down(N, q).astype(BF16)
            rsend(pnear, rdir, q, ro_recv.at[q])

    def far(q):
        o, w = out[q]
        with scope("far%d" % q):
            pfar[:, pl.ds(o, w)] = down(F, q).astype(BF16)
            rsend(pfar, rfar, q, rf_recv.at[q])

    def combine(q):
        o, w = out[q]
        sl = pl.ds(o, w)
        with scope("comb%d" % q):
            part = down(M, q)
        with scope("S1w%d" % q):
            wait_bytes(X.at[pl.ds(0, 2 * half), sl], rf_recv.at[q])
        for j in range(2):
            pcomb[pl.ds(j * half, half), sl] = (part[j * half:(j + 1) * half] + rfar[j, :, sl].astype(F32)).astype(BF16)
        rsend(pcomb, rcomb, q, ro_recv.at[q])

    def finish(q):
        o, w = out[q]
        sl = pl.ds(o, w)
        mine = down(O, q)
        with scope("S3w%d" % q):
            wait_bytes(X.at[pl.ds(0, 4 * half), sl], ro_recv.at[q])
        y_lo = mine[:half] + rcomb[0, :, sl].astype(F32) + rdir[1, :, sl].astype(F32)
        y_hi = mine[half:] + rcomb[1, :, sl].astype(F32) + rdir[0, :, sl].astype(F32)
        y = jnp.concatenate([y_lo.astype(BF16), y_hi.astype(BF16)], axis=0)
        sp = pl.ds(o, packed(w))
        sr[:, sp] = pack(p2t_ref, y)
        for k in range(1, n_ep):
            dst_e = lax.rem(ep + k, n_ep)
            send(sr.at[rows(dst_e * 16, 16), sp], rr.at[rows(ep * 16, 16), sp], C_S, c_recv.at[q], edev(k))
        rr[rows(ep * 16, 16), sp] = sr[rows(ep * 16, 16), sp]

    def give_back(q):
        o, w = out[q]
        sl = pl.ds(o, w)
        with scope("RBw%d" % q):
            wait_bytes(rr.at[pl.ds(0, others), pl.ds(o, packed(w))], c_recv.at[q])
        ts[:, sl] = unpack(p1t_ref, rr[:, pl.ds(o, packed(w))], w)
        for k in (2, 1, 3):
            dst_x = lax.rem(x + k, RING)
            send(ts.at[rows(dst_x * slots, slots), sl], ret_ref.at[:, cols(x * D4 + o, w)], E_S, d_recv, xdev(k))
        ret_ref[:, cols(x * D4 + o, w)] = ts[rows(x * slots, slots), sl]

    first(N)
    with scope("zfwait"):
        for q in range(C):
            zwait(zf_recv.at[q], q, 2)
    first(F)
    second(N)
    second(F)
    send_down(1)
    send_down(2)
    hwait(N)
    dwait(0)
    near(0)
    hwait(F)
    far(0)
    with scope("zmwait"):
        for q in range(C):
            zwait(zm_recv.at[q], q, 2)
    first(M)
    for q in range(3, Q):
        send_down(q)
    for q in (1, 2):
        dwait(q)
        near(q)
        far(q)
    second(M)
    first(O)
    for q in range(3, Q):
        dwait(q)
        near(q)
        far(q)
    second(O)
    hwait(M)
    for q in range(Q):
        combine(q)
    hwait(O)
    for q in range(Q):
        finish(q)
    for q in range(Q):
        give_back(q)
    with scope("RAw"):
        wait_bytes(ts.at[pl.ds(0, (RING - 1) * slots), :], d_recv)
    with scope("sends"):
        for group, ref in ((A_S, bs), (W_S, wgu.at[pl.ds(0, RING - 1)]),
                           (D_S, wd.at[pl.ds(0, (RING - 1) * inner), :]),
                           (B_S, sb.at[pl.ds(0, others), pl.ds(0, sum(packed(w) for _, w in into))]), (Z_S, X.at[pl.ds(0, 6 * half), :]),
                           (G_S, hr), (H_S, H.at[:, :, pl.ds(0, (RING - 1) * inner)]),
                           (R_S, X.at[pl.ds(0, 6 * half), :]), (C_S, sr.at[pl.ds(0, others), pl.ds(0, sum(packed(w) for _, w in out))]),
                           (E_S, ts.at[pl.ds(0, (RING - 1) * slots), :])):
            wait_bytes(ref, send_sem.at[group])


def body(tokens, expert_ids, gate_q, w_gate, w_up, w_down):
    n_ep = lax.axis_size("ep")
    T, width = tokens.shape
    D4 = width // RING
    slots = n_ep * CAP
    R = slots * RING
    inner = w_down.shape[1]
    per = CAP * RING

    p1 = np.zeros((1 + CAP, n_ep * 16, R), np.float32)
    p2 = np.zeros((1 + CAP, R, n_ep * 16), np.float32)
    for e in range(n_ep):
        for s in range(RING):
            for q in range(CAP):
                j = s * CAP + q
                p1[0, e * 16 + j, s * slots + e * CAP + q] = 1
                p1[1 + q, e * 16 + per + s, s * slots + e * CAP + q] = 1
                p2[0, e * per + j, e * 16 + j] = 1
                p2[1 + q, e * per + j, e * 16 + per + s] = 1
    consts = [jnp.asarray(m, BF16) for m in (p1, p1.transpose(0, 2, 1), p2, p2.transpose(0, 2, 1))]

    vm = pl.BlockSpec(memory_space=pltpu.VMEM)
    anyspec = pl.BlockSpec(memory_space=pl.ANY)
    V = pltpu.VMEM
    DMA = pltpu.SemaphoreType.DMA
    half = R // 2
    C, Q = len(CIN), len(CHUNKS)
    scratch = [
        V((expert_ids.shape[1], T), jnp.int32), V((expert_ids.shape[1], T), jnp.int32),
    ] + [V(m.shape, BF16) for m in consts] + [
        V((T, width), BF16),
        V((3, slots, D4), BF16),
        V((R, D4), BF16),
        V((n_ep * 16, D4), BF16),
        V((n_ep * 16, D4), BF16),
        V((RING * R, D4), BF16),
        V((RING, D4, 2 * inner), BF16),
        V((RING * inner, D4), BF16),
        V((RING, 3, R, 2 * inner), BF16),
        V((RING, R, 2 * inner), F32),
        V((RING, 3, R, 2 * inner), BF16),
        V((RING, R, RING * inner), BF16),
        V((R, D4), BF16),
        V((R, D4), BF16),
        V((R, D4), BF16),
        V((2, half, D4), BF16),
        V((2, half, D4), BF16),
        V((2, half, D4), BF16),
        V((n_ep * 16, D4), BF16),
        V((n_ep * 16, D4), BF16),
        V((R, D4), BF16),
        DMA((9 + Q,)), DMA((10,)), DMA(()), DMA((Q,)), DMA((C,)), DMA((C,)), DMA((C, 2)), DMA((C,)), DMA((C,)),
        DMA((4,)), DMA((4,)), DMA((Q,)), DMA((Q,)), DMA((Q,)), DMA(()),
    ]
    ret, scal = pl.pallas_call(
        kernel,
        out_shape=(pltpu.VMEM((slots, width), BF16), pltpu.VMEM((slots, T), BF16)),
        in_specs=[anyspec] * 10,
        out_specs=(vm, vm),
        scratch_shapes=scratch,
        compiler_params=pltpu.CompilerParams(collective_id=0, has_side_effects=True, vmem_limit_bytes=60 * 1024 * 1024),
        name="experts",
    )(expert_ids.T, gate_q.T, *consts, tokens, w_gate, w_up, w_down)
    mixed = lax.dot_general(scal, ret, (((0,), (0,)), ((), ())), preferred_element_type=F32)
    return mixed.astype(BF16)


def solution(mesh):
    in_specs = (
        P(("ep", "etp"), None),
        P(("ep", "etp"), None),
        P(("ep", "etp"), None),
        P("ep", None, "etp"),
        P("ep", None, "etp"),
        P("ep", "etp", None),
    )
    out_specs = P(("ep", "etp"), None)
    return jax.shard_map(body, mesh=mesh, in_specs=in_specs, out_specs=out_specs, check_vma=False)
```

```python
import jax
import jax.numpy as jnp
import numpy as np
from jax import lax
from jax.experimental import pallas as pl
from jax.experimental.pallas import tpu as pltpu
from jax.sharding import PartitionSpec as P

CAP = 3
RING = 4
CIN = (4, 4, 4, 2)
CHUNKS = (4, 4, 4, 2)
MESH = pl.DeviceIdType.MESH
F32 = jnp.float32
BF16 = jnp.bfloat16
scope = jax.named_scope


def third(c):
    return lax.shift_right_logical(c * 43691, 17)


def dot(a, b):
    return jnp.dot(a, b, preferred_element_type=F32)


def packed(width):
    return width * 3 // 4 if width % 512 == 0 else width


def pack(p, src):
    w = src.shape[1]
    keep = packed(w)
    made = dot(p[0], src[:, :keep])
    if keep < w:
        made = made + jnp.concatenate([dot(p[1 + j], src[:, keep:]) for j in range(3)], axis=1)
    return made.astype(BF16)


def unpack(p, src, w):
    keep = packed(w)
    made = dot(p[0], src).astype(BF16)
    if keep < w:
        part = w - keep
        rest = dot(p[1], src[:, :part]) + dot(p[2], src[:, part:2 * part]) + dot(p[3], src[:, 2 * part:])
        made = jnp.concatenate([made, rest.astype(BF16)], axis=1)
    return made


def kernel(ids_hbm, gate_hbm, p1_hbm, p1t_hbm, p2_hbm, p2t_hbm, tok_hbm, wg_hbm, wu_hbm, wd_hbm,
           mixed_ref,
           ret_ref, scal_ref, ids_ref, gate_ref, p1_ref, p1t_ref, p2_ref, p2t_ref, tok, bs, xa, sb, rb, X, wgu, wd, gp, own, hr, H, pfar, pnear, pcomb, rfar, rdir, rcomb,
           sr, rr, ts,
           loc_sem, send_sem, w_recv, wd_recv, a_recv, b_recv, zn_recv, zf_recv, zm_recv, g_recv,
           h_recv, rf_recv, ro_recv, c_recv, d_recv):
    ep = lax.axis_index("ep")
    etp = lax.axis_index("etp")
    n_ep = lax.axis_size("ep")
    zi = etp // RING
    x = etp % RING
    width = tok.shape[1]
    D4 = width // RING
    slots = n_ep * CAP
    R = slots * RING
    half = R // 2
    inner = wd.shape[0] // RING

    def xdev(k):
        return (ep, zi * RING + lax.rem(x + k, RING))

    def zdev(k):
        return (ep, lax.rem(zi + k, RING) * RING + x)

    def edev(k):
        return (lax.rem(ep + k, n_ep), etp)

    def spans(parts):
        made = []
        for n in parts:
            made.append((sum(w for _, w in made), n * D4 // sum(parts)))
        return made

    into, out = spans(CIN), spans(CHUNKS)
    C, Q = len(into), len(out)
    others = (n_ep - 1) * 16

    A_S, W_S, D_S, B_S, Z_S, G_S, H_S, R_S, C_S, E_S = range(10)

    def send(src, dst, group, rsem, dev):
        pltpu.make_async_remote_copy(src_ref=src, dst_ref=dst, send_sem=send_sem.at[group], recv_sem=rsem,
                                     device_id=dev, device_id_type=MESH).start()

    def wait_bytes(ref, sem):
        pltpu.make_async_copy(ref, ref, sem).wait()

    def rows(start, size):
        return pl.ds(pl.multiple_of(start, 16), size)

    def cols(start, size):
        return pl.ds(pl.multiple_of(start, 128), size)

    barrier = pltpu.get_barrier_semaphore()
    for k in range(1, RING):
        pl.semaphore_signal(barrier, inc=1, device_id=xdev(k), device_id_type=MESH)
    for k in (1, RING - 1):
        pl.semaphore_signal(barrier, inc=1, device_id=zdev(k), device_id_type=MESH)
    for k in range(1, n_ep):
        pl.semaphore_signal(barrier, inc=1, device_id=edev(k), device_id_type=MESH)

    ids_copies = [pltpu.make_async_copy(ids_hbm, ids_ref, loc_sem.at[0]),
                  pltpu.make_async_copy(gate_hbm, gate_ref, loc_sem.at[1])]
    tok_copy = pltpu.make_async_copy(tok_hbm, tok, loc_sem.at[2])
    p_copies = [pltpu.make_async_copy(src, dst, loc_sem.at[3 + i])
                for i, (src, dst) in enumerate(((p1_hbm, p1_ref), (p1t_hbm, p1t_ref), (p2_hbm, p2_ref), (p2t_hbm, p2t_ref)))]
    for cp in ids_copies + [tok_copy] + p_copies:
        cp.start()
    w_loc = [
        pltpu.make_async_copy(wg_hbm.at[0, rows(x * D4, D4), :], wgu.at[x, :, pl.ds(0, inner)], loc_sem.at[7]),
        pltpu.make_async_copy(wu_hbm.at[0, rows(x * D4, D4), :], wgu.at[x, :, pl.ds(inner, inner)], loc_sem.at[8]),
    ] + [
        pltpu.make_async_copy(wd_hbm.at[0, :, cols(x * D4 + o, w)], wd.at[rows(x * inner, inner), pl.ds(o, w)], loc_sem.at[9 + q])
        for q, (o, w) in enumerate(out)
    ]

    with scope("idswait"):
        for cp in ids_copies:
            cp.wait()

    T = tok.shape[0]
    c = lax.broadcasted_iota(jnp.int32, (slots, T), 0)
    expert = third(c)
    slot = (c - CAP * expert).astype(F32)
    hot = jnp.zeros((slots, T), F32)
    weight = jnp.zeros((slots, T), F32)
    for r in range(ids_ref.shape[0]):
        eq = ids_ref[r:r + 1, :] == expert
        hot = jnp.where(eq, 1.0, hot)
        weight = jnp.where(eq, gate_ref[r:r + 1, :].astype(F32), weight)
    before = lax.broadcasted_iota(jnp.int32, (T, T), 0) < lax.broadcasted_iota(jnp.int32, (T, T), 1)
    earlier = dot(hot.astype(BF16), jnp.where(before, 1.0, 0.0).astype(BF16))
    placing = jnp.where(earlier == slot, hot, 0.0)
    scal_ref[...] = (placing * weight * (1.0 / 1024.0)).T.astype(BF16)
    placing = placing.astype(BF16)

    with scope("tokwait"):
        tok_copy.wait()
    def bucket(q):
        o, w = into[q]
        for k in (2, 1, 3, 0):
            piece = dot(placing, tok[:, cols(lax.rem(x + k, RING) * D4 + o, w)]).astype(BF16)
            if k == 0:
                xa[rows(x * slots, slots), pl.ds(o, w)] = piece
            else:
                bs[k - 1, :, pl.ds(o, w)] = piece

    for q in range(C):
        bucket(q)
    with scope("barrier_in"):
        pl.semaphore_wait(barrier, (RING - 1) + 2 + (n_ep - 1))
    for q, (o, w) in enumerate(into):
        for k in (2, 1, 3):
            send(bs.at[k - 1, :, pl.ds(o, w)], xa.at[rows(x * slots, slots), pl.ds(o, w)],
                 A_S, a_recv.at[q], xdev(k))

    for k in (1, 3, 2):
        dst_x = lax.rem(x + k, RING)
        send(wg_hbm.at[0, rows(dst_x * D4, D4), :], wgu.at[x, :, pl.ds(0, inner)], W_S, w_recv, xdev(k))
        send(wu_hbm.at[0, rows(dst_x * D4, D4), :], wgu.at[x, :, pl.ds(inner, inner)], W_S, w_recv, xdev(k))

    def send_down(q):
        o, w = out[q]
        for k in (1, 3, 2):
            dst_x = lax.rem(x + k, RING)
            send(wd_hbm.at[0, :, cols(dst_x * D4 + o, w)], wd.at[rows(x * inner, inner), pl.ds(o, w)],
                 D_S, wd_recv.at[q], xdev(k))

    send_down(0)
    for cp in w_loc:
        cp.start()

    for cp in p_copies:
        cp.wait()

    for q, (o, w) in enumerate(into):
        sl = pl.ds(o, w)
        sp = pl.ds(o, packed(w))
        with scope("A_wait"):
            wait_bytes(xa.at[pl.ds(0, (RING - 1) * slots), sl], a_recv.at[q])
        sb[:, sp] = pack(p1_ref, xa[:, sl])
        for k in range(1, n_ep):
            dst_e = lax.rem(ep + k, n_ep)
            send(sb.at[rows(dst_e * 16, 16), sp], rb.at[rows(ep * 16, 16), sp], B_S, b_recv.at[q], edev(k))
        rb[rows(ep * 16, 16), sp] = sb[rows(ep * 16, 16), sp]

    zm = lax.rem(zi + RING - 1, RING)
    zp = lax.rem(zi + 1, RING)
    zf = lax.rem(zi + 2, RING)

    def unit(b, h):
        return rows((2 * b + h) * half, half)

    def zsend(q, b, h, rsem, k):
        part = X.at[unit(b, h), pl.ds(*into[q])]
        send(part, part, Z_S, rsem, zdev(k))

    def zwait(sem, q, count):
        wait_bytes(X.at[pl.ds(0, count * half), pl.ds(*into[q])], sem)

    UP, DOWN = 1, RING - 1

    def outset(q):
        o, w = into[q]
        sp = pl.ds(o, packed(w))
        with scope("B_wait"):
            wait_bytes(rb.at[pl.ds(0, others), sp], b_recv.at[q])
        X[rows(zi * R, R), pl.ds(o, w)] = unpack(p2_ref, rb[:, sp], w)
        zsend(q, zi, 0, zn_recv.at[q, 0], UP)
        zsend(q, zi, 1, zn_recv.at[q, 1], DOWN)

    def forward(q):
        with scope("Z0_wait"):
            zwait(zn_recv.at[q, 0], q, 1)
        zsend(q, zm, 0, zf_recv.at[q], UP)
        with scope("Z3_wait"):
            zwait(zn_recv.at[q, 1], q, 1)
        zsend(q, zp, 1, zf_recv.at[q], DOWN)

    for q in range(C):
        outset(q)
    for q in range(C):
        forward(q)
    for q in range(C):
        zsend(q, zi, 1, zm_recv.at[q], UP)
        zsend(q, zi, 0, zm_recv.at[q], DOWN)

    with scope("W_wait"):
        wait_bytes(wgu.at[pl.ds(0, RING - 1)], w_recv)
        w_loc[0].wait()
        w_loc[1].wait()

    N, F, M, O = range(4)
    pairs = [((zp, 1), (zm, 0)), ((zf, 0), (zf, 1)), ((zp, 0), (zm, 1)), ((zi, 0), (zi, 1))]
    def first(i):
        with scope("first%d" % i):
            xs = jnp.concatenate([X[unit(*u), :] for u in pairs[i]], axis=0)
            for k in (2, 1, 3, 0):
                dst_x = lax.rem(x + k, RING)
                acc = dot(xs, wgu[dst_x])
                if k == 0:
                    own[i] = acc
                else:
                    gp[i, k - 1] = acc.astype(BF16)
                    send(gp.at[i, k - 1], hr.at[i, k - 1], G_S, g_recv.at[i], xdev(k))

    def second(i):
        with scope("gwait%d" % i):
            wait_bytes(hr.at[i], g_recv.at[i])
        with scope("second%d" % i):
            total = own[i]
            for k in range(RING - 1):
                total = total + hr[i, k].astype(F32)
            g = total[:, :inner]
            u = total[:, inner:]
            part = H.at[i, :, cols(x * inner, inner)]
            part[...] = (g / (1.0 + jnp.exp(-g)) * u).astype(BF16)
            for k in (2, 1, 3):
                send(part, part, H_S, h_recv.at[i], xdev(k))

    def hwait(i):
        with scope("hwait%d" % i):
            wait_bytes(H.at[i, :, pl.ds(0, (RING - 1) * inner)], h_recv.at[i])

    def dwait(q):
        with scope("dwait%d" % q):
            wait_bytes(wd.at[pl.ds(0, (RING - 1) * inner), pl.ds(*out[q])], wd_recv.at[q])
            w_loc[2 + q].wait()

    def down(i, q):
        o, w = out[q]
        return dot(H[i], wd[:, pl.ds(o, w)])

    def rsend(buf, into, q, rsem):
        o, w = out[q]
        for j, k in ((0, UP), (1, DOWN)):
            send(buf.at[pl.ds(j * half, half), pl.ds(o, w)], into.at[j, :, pl.ds(o, w)], R_S, rsem, zdev(k))

    def near(q):
        o, w = out[q]
        with scope("near%d" % q):
            pnear[:, pl.ds(o, w)] = down(N, q).astype(BF16)
            rsend(pnear, rdir, q, ro_recv.at[q])

    def far(q):
        o, w = out[q]
        with scope("far%d" % q):
            pfar[:, pl.ds(o, w)] = down(F, q).astype(BF16)
            rsend(pfar, rfar, q, rf_recv.at[q])

    def combine(q):
        o, w = out[q]
        sl = pl.ds(o, w)
        with scope("comb%d" % q):
            part = down(M, q)
        with scope("S1w%d" % q):
            wait_bytes(X.at[pl.ds(0, 2 * half), sl], rf_recv.at[q])
        for j in range(2):
            pcomb[pl.ds(j * half, half), sl] = (part[j * half:(j + 1) * half] + rfar[j, :, sl].astype(F32)).astype(BF16)
        rsend(pcomb, rcomb, q, ro_recv.at[q])

    def finish(q):
        o, w = out[q]
        sl = pl.ds(o, w)
        mine = down(O, q)
        with scope("S3w%d" % q):
            wait_bytes(X.at[pl.ds(0, 4 * half), sl], ro_recv.at[q])
        y_lo = mine[:half] + rcomb[0, :, sl].astype(F32) + rdir[1, :, sl].astype(F32)
        y_hi = mine[half:] + rcomb[1, :, sl].astype(F32) + rdir[0, :, sl].astype(F32)
        y = jnp.concatenate([y_lo.astype(BF16), y_hi.astype(BF16)], axis=0)
        sp = pl.ds(o, packed(w))
        sr[:, sp] = pack(p2t_ref, y)
        for k in range(1, n_ep):
            dst_e = lax.rem(ep + k, n_ep)
            send(sr.at[rows(dst_e * 16, 16), sp], rr.at[rows(ep * 16, 16), sp], C_S, c_recv.at[q], edev(k))
        rr[rows(ep * 16, 16), sp] = sr[rows(ep * 16, 16), sp]

    def give_back(q):
        o, w = out[q]
        sl = pl.ds(o, w)
        with scope("RBw%d" % q):
            wait_bytes(rr.at[pl.ds(0, others), pl.ds(o, packed(w))], c_recv.at[q])
        ts[:, sl] = unpack(p1t_ref, rr[:, pl.ds(o, packed(w))], w)
        for k in (2, 1, 3):
            dst_x = lax.rem(x + k, RING)
            send(ts.at[rows(dst_x * slots, slots), sl], ret_ref.at[:, cols(x * D4 + o, w)], E_S, d_recv.at[q], xdev(k))
        ret_ref[:, cols(x * D4 + o, w)] = ts[rows(x * slots, slots), sl]

    first(N)
    with scope("zfwait"):
        for q in range(C):
            zwait(zf_recv.at[q], q, 2)
    first(F)
    second(N)
    second(F)
    send_down(1)
    send_down(2)
    hwait(N)
    dwait(0)
    near(0)
    hwait(F)
    far(0)
    with scope("zmwait"):
        for q in range(C):
            zwait(zm_recv.at[q], q, 2)
    first(M)
    for q in range(3, Q):
        send_down(q)
    for q in (1, 2):
        dwait(q)
        near(q)
        far(q)
    second(M)
    first(O)
    for q in range(3, Q):
        dwait(q)
        near(q)
        far(q)
    second(O)
    hwait(M)
    for q in range(Q):
        combine(q)
    hwait(O)
    for q in range(Q):
        finish(q)
    for q in range(Q):
        give_back(q)
    for q, (o, w) in enumerate(out):
        with scope("RAw%d" % q):
            wait_bytes(ts.at[pl.ds(0, (RING - 1) * slots), pl.ds(o, w)], d_recv.at[q])
        for j in range(RING):
            sl = pl.ds(j * D4 + o, w)
            mixed_ref[:, sl] = dot(scal_ref[...], ret_ref[:, sl]).astype(BF16)
    with scope("sends"):
        for group, ref in ((A_S, bs), (W_S, wgu.at[pl.ds(0, RING - 1)]),
                           (D_S, wd.at[pl.ds(0, (RING - 1) * inner), :]),
                           (B_S, sb.at[pl.ds(0, others), pl.ds(0, sum(packed(w) for _, w in into))]), (Z_S, X.at[pl.ds(0, 6 * half), :]),
                           (G_S, hr), (H_S, H.at[:, :, pl.ds(0, (RING - 1) * inner)]),
                           (R_S, X.at[pl.ds(0, 6 * half), :]), (C_S, sr.at[pl.ds(0, others), pl.ds(0, sum(packed(w) for _, w in out))]),
                           (E_S, ts.at[pl.ds(0, (RING - 1) * slots), :])):
            wait_bytes(ref, send_sem.at[group])


def body(tokens, expert_ids, gate_q, w_gate, w_up, w_down):
    n_ep = lax.axis_size("ep")
    T, width = tokens.shape
    D4 = width // RING
    slots = n_ep * CAP
    R = slots * RING
    inner = w_down.shape[1]
    per = CAP * RING

    p1 = np.zeros((1 + CAP, n_ep * 16, R), np.float32)
    p2 = np.zeros((1 + CAP, R, n_ep * 16), np.float32)
    for e in range(n_ep):
        for s in range(RING):
            for q in range(CAP):
                j = s * CAP + q
                p1[0, e * 16 + j, s * slots + e * CAP + q] = 1
                p1[1 + q, e * 16 + per + s, s * slots + e * CAP + q] = 1
                p2[0, e * per + j, e * 16 + j] = 1
                p2[1 + q, e * per + j, e * 16 + per + s] = 1
    consts = [jnp.asarray(m, BF16) for m in (p1, p1.transpose(0, 2, 1), p2, p2.transpose(0, 2, 1))]

    vm = pl.BlockSpec(memory_space=pltpu.VMEM)
    anyspec = pl.BlockSpec(memory_space=pl.ANY)
    V = pltpu.VMEM
    DMA = pltpu.SemaphoreType.DMA
    half = R // 2
    C, Q = len(CIN), len(CHUNKS)
    scratch = [
        V((slots, width), BF16), V((T, slots), BF16),
        V((expert_ids.shape[1], T), jnp.int32), V((expert_ids.shape[1], T), jnp.int32),
    ] + [V(m.shape, BF16) for m in consts] + [
        V((T, width), BF16),
        V((3, slots, D4), BF16),
        V((R, D4), BF16),
        V((n_ep * 16, D4), BF16),
        V((n_ep * 16, D4), BF16),
        V((RING * R, D4), BF16),
        V((RING, D4, 2 * inner), BF16),
        V((RING * inner, D4), BF16),
        V((RING, 3, R, 2 * inner), BF16),
        V((RING, R, 2 * inner), F32),
        V((RING, 3, R, 2 * inner), BF16),
        V((RING, R, RING * inner), BF16),
        V((R, D4), BF16),
        V((R, D4), BF16),
        V((R, D4), BF16),
        V((2, half, D4), BF16),
        V((2, half, D4), BF16),
        V((2, half, D4), BF16),
        V((n_ep * 16, D4), BF16),
        V((n_ep * 16, D4), BF16),
        V((R, D4), BF16),
        DMA((9 + Q,)), DMA((10,)), DMA(()), DMA((Q,)), DMA((C,)), DMA((C,)), DMA((C, 2)), DMA((C,)), DMA((C,)),
        DMA((4,)), DMA((4,)), DMA((Q,)), DMA((Q,)), DMA((Q,)), DMA((Q,)),
    ]
    return pl.pallas_call(
        kernel,
        out_shape=pltpu.VMEM((T, width), BF16),
        in_specs=[anyspec] * 10,
        out_specs=vm,
        scratch_shapes=scratch,
        compiler_params=pltpu.CompilerParams(collective_id=0, has_side_effects=True, vmem_limit_bytes=60 * 1024 * 1024),
        name="experts",
    )(expert_ids.T, gate_q.T, *consts, tokens, w_gate, w_up, w_down)


def solution(mesh):
    in_specs = (
        P(("ep", "etp"), None),
        P(("ep", "etp"), None),
        P(("ep", "etp"), None),
        P("ep", None, "etp"),
        P("ep", None, "etp"),
        P("ep", "etp", None),
    )
    out_specs = P(("ep", "etp"), None)
    return jax.shard_map(body, mesh=mesh, in_specs=in_specs, out_specs=out_specs, check_vma=False)
```

```python
import jax
import jax.numpy as jnp
import numpy as np
from jax import lax
from jax.experimental import pallas as pl
from jax.experimental.pallas import tpu as pltpu
from jax.sharding import PartitionSpec as P

CAP = 3
RING = 4
CIN = (4, 4, 4, 2)
CHUNKS = (4, 4, 4, 2)
MESH = pl.DeviceIdType.MESH
F32 = jnp.float32
BF16 = jnp.bfloat16
scope = jax.named_scope


def third(c):
    return lax.shift_right_logical(c * 43691, 17)


def dot(a, b):
    return jnp.dot(a, b, preferred_element_type=F32)


def packed(width):
    return width * 3 // 4 if width % 512 == 0 else width


def pack(p, src):
    w = src.shape[1]
    keep = packed(w)
    made = dot(p[0], src[:, :keep])
    if keep < w:
        made = made + jnp.concatenate([dot(p[1 + j], src[:, keep:]) for j in range(3)], axis=1)
    return made.astype(BF16)


def unpack(p, src, w):
    keep = packed(w)
    made = dot(p[0], src).astype(BF16)
    if keep < w:
        part = w - keep
        rest = dot(p[1], src[:, :part]) + dot(p[2], src[:, part:2 * part]) + dot(p[3], src[:, 2 * part:])
        made = jnp.concatenate([made, rest.astype(BF16)], axis=1)
    return made


def kernel(ids_hbm, gate_hbm, p1_hbm, p1t_hbm, p2_hbm, p2t_hbm, tok_hbm, wg_hbm, wu_hbm, wd_hbm,
           mixed_ref,
           ret_ref, scal_ref, ids_ref, gate_ref, p1_ref, p1t_ref, p2_ref, p2t_ref, tok, bs, xa, sb, rb, X, wgu, wd, gp, own, hr, H, pfar, pnear, pcomb, rfar, rdir, rcomb,
           sr, rr, ts,
           loc_sem, send_sem, w_recv, wd_recv, a_recv, b_recv, zn_recv, zf_recv, zm_recv, g_recv,
           h_recv, rf_recv, ro_recv, c_recv, d_recv):
    ep = lax.axis_index("ep")
    etp = lax.axis_index("etp")
    n_ep = lax.axis_size("ep")
    zi = etp // RING
    x = etp % RING
    width = tok.shape[1]
    D4 = width // RING
    slots = n_ep * CAP
    R = slots * RING
    half = R // 2
    inner = wd.shape[0] // RING

    def xdev(k):
        return (ep, zi * RING + lax.rem(x + k, RING))

    def zdev(k):
        return (ep, lax.rem(zi + k, RING) * RING + x)

    def edev(k):
        return (lax.rem(ep + k, n_ep), etp)

    def spans(parts):
        made = []
        for n in parts:
            made.append((sum(w for _, w in made), n * D4 // sum(parts)))
        return made

    into, out = spans(CIN), spans(CHUNKS)
    C, Q = len(into), len(out)
    others = (n_ep - 1) * 16

    A_S, W_S, D_S, B_S, Z_S, G_S, H_S, R_S, C_S, E_S = range(10)

    def send(src, dst, group, rsem, dev):
        pltpu.make_async_remote_copy(src_ref=src, dst_ref=dst, send_sem=send_sem.at[group], recv_sem=rsem,
                                     device_id=dev, device_id_type=MESH).start()

    def wait_bytes(ref, sem):
        pltpu.make_async_copy(ref, ref, sem).wait()

    def rows(start, size):
        return pl.ds(pl.multiple_of(start, 16), size)

    def cols(start, size):
        return pl.ds(pl.multiple_of(start, 128), size)

    barrier = pltpu.get_barrier_semaphore()
    for k in range(1, RING):
        pl.semaphore_signal(barrier, inc=1, device_id=xdev(k), device_id_type=MESH)
    for k in (1, RING - 1):
        pl.semaphore_signal(barrier, inc=1, device_id=zdev(k), device_id_type=MESH)
    for k in range(1, n_ep):
        pl.semaphore_signal(barrier, inc=1, device_id=edev(k), device_id_type=MESH)

    ids_copies = [pltpu.make_async_copy(ids_hbm, ids_ref, loc_sem.at[0]),
                  pltpu.make_async_copy(gate_hbm, gate_ref, loc_sem.at[1])]
    tok_copy = pltpu.make_async_copy(tok_hbm, tok, loc_sem.at[2])
    p_copies = [pltpu.make_async_copy(src, dst, loc_sem.at[3 + i])
                for i, (src, dst) in enumerate(((p1_hbm, p1_ref), (p1t_hbm, p1t_ref), (p2_hbm, p2_ref), (p2t_hbm, p2t_ref)))]
    for cp in ids_copies + [tok_copy] + p_copies:
        cp.start()
    w_loc = [
        pltpu.make_async_copy(wg_hbm.at[0, rows(x * D4, D4), :], wgu.at[x, :, pl.ds(0, inner)], loc_sem.at[7]),
        pltpu.make_async_copy(wu_hbm.at[0, rows(x * D4, D4), :], wgu.at[x, :, pl.ds(inner, inner)], loc_sem.at[8]),
    ] + [
        pltpu.make_async_copy(wd_hbm.at[0, :, cols(x * D4 + o, w)], wd.at[rows(x * inner, inner), pl.ds(o, w)], loc_sem.at[9 + q])
        for q, (o, w) in enumerate(out)
    ]

    with scope("idswait"):
        for cp in ids_copies:
            cp.wait()

    T = tok.shape[0]
    c = lax.broadcasted_iota(jnp.int32, (slots, T), 0)
    expert = third(c)
    slot = (c - CAP * expert).astype(F32)
    hot = jnp.zeros((slots, T), F32)
    weight = jnp.zeros((slots, T), F32)
    for r in range(ids_ref.shape[0]):
        eq = ids_ref[r:r + 1, :] == expert
        hot = jnp.where(eq, 1.0, hot)
        weight = jnp.where(eq, gate_ref[r:r + 1, :].astype(F32), weight)
    before = lax.broadcasted_iota(jnp.int32, (T, T), 0) < lax.broadcasted_iota(jnp.int32, (T, T), 1)
    earlier = dot(hot.astype(BF16), jnp.where(before, 1.0, 0.0).astype(BF16))
    placing = jnp.where(earlier == slot, hot, 0.0)
    scal_ref[...] = (placing * weight * (1.0 / 1024.0)).T.astype(BF16)
    placing = placing.astype(BF16)

    with scope("tokwait"):
        tok_copy.wait()
    def bucket(q):
        o, w = into[q]
        for k in (2, 1, 3, 0):
            piece = dot(placing, tok[:, cols(lax.rem(x + k, RING) * D4 + o, w)]).astype(BF16)
            if k == 0:
                xa[rows(x * slots, slots), pl.ds(o, w)] = piece
            else:
                bs[k - 1, :, pl.ds(o, w)] = piece

    for q in range(C):
        bucket(q)
    with scope("barrier_in"):
        pl.semaphore_wait(barrier, (RING - 1) + 2 + (n_ep - 1))
    for q, (o, w) in enumerate(into):
        for k in (2, 1, 3):
            send(bs.at[k - 1, :, pl.ds(o, w)], xa.at[rows(x * slots, slots), pl.ds(o, w)],
                 A_S, a_recv.at[q], xdev(k))

    for k in (1, 3, 2):
        dst_x = lax.rem(x + k, RING)
        send(wg_hbm.at[0, rows(dst_x * D4, D4), :], wgu.at[x, :, pl.ds(0, inner)], W_S, w_recv, xdev(k))
        send(wu_hbm.at[0, rows(dst_x * D4, D4), :], wgu.at[x, :, pl.ds(inner, inner)], W_S, w_recv, xdev(k))

    def send_down(q):
        o, w = out[q]
        for k in (1, 3, 2):
            dst_x = lax.rem(x + k, RING)
            send(wd_hbm.at[0, :, cols(dst_x * D4 + o, w)], wd.at[rows(x * inner, inner), pl.ds(o, w)],
                 D_S, wd_recv.at[q], xdev(k))

    send_down(0)
    for cp in w_loc:
        cp.start()

    for cp in p_copies:
        cp.wait()

    for q, (o, w) in enumerate(into):
        sl = pl.ds(o, w)
        sp = pl.ds(o, packed(w))
        with scope("A_wait"):
            wait_bytes(xa.at[pl.ds(0, (RING - 1) * slots), sl], a_recv.at[q])
        sb[:, sp] = pack(p1_ref, xa[:, sl])
        for k in range(1, n_ep):
            dst_e = lax.rem(ep + k, n_ep)
            send(sb.at[rows(dst_e * 16, 16), sp], rb.at[rows(ep * 16, 16), sp], B_S, b_recv.at[q], edev(k))
        rb[rows(ep * 16, 16), sp] = sb[rows(ep * 16, 16), sp]

    zm = lax.rem(zi + RING - 1, RING)
    zp = lax.rem(zi + 1, RING)
    zf = lax.rem(zi + 2, RING)

    def unit(b, h):
        return rows((2 * b + h) * half, half)

    def zsend(q, b, h, rsem, k):
        part = X.at[unit(b, h), pl.ds(*into[q])]
        send(part, part, Z_S, rsem, zdev(k))

    def zwait(sem, q, count):
        wait_bytes(X.at[pl.ds(0, count * half), pl.ds(*into[q])], sem)

    UP, DOWN = 1, RING - 1

    def outset(q):
        o, w = into[q]
        sp = pl.ds(o, packed(w))
        with scope("B_wait"):
            wait_bytes(rb.at[pl.ds(0, others), sp], b_recv.at[q])
        X[rows(zi * R, R), pl.ds(o, w)] = unpack(p2_ref, rb[:, sp], w)
        zsend(q, zi, 0, zn_recv.at[q, 0], UP)
        zsend(q, zi, 1, zn_recv.at[q, 1], DOWN)

    def forward(q):
        with scope("Z0_wait"):
            zwait(zn_recv.at[q, 0], q, 1)
        zsend(q, zm, 0, zf_recv.at[q], UP)
        with scope("Z3_wait"):
            zwait(zn_recv.at[q, 1], q, 1)
        zsend(q, zp, 1, zf_recv.at[q], DOWN)

    for q in range(C):
        outset(q)
    for q in range(C):
        forward(q)
    for q in range(C):
        zsend(q, zi, 1, zm_recv.at[q], UP)
        zsend(q, zi, 0, zm_recv.at[q], DOWN)

    with scope("W_wait"):
        wait_bytes(wgu.at[pl.ds(0, RING - 1)], w_recv)
        w_loc[0].wait()
        w_loc[1].wait()

    N, F, M, O = range(4)
    pairs = [((zp, 1), (zm, 0)), ((zf, 0), (zf, 1)), ((zp, 0), (zm, 1)), ((zi, 0), (zi, 1))]
    def first(i):
        with scope("first%d" % i):
            xs = jnp.concatenate([X[unit(*u), :] for u in pairs[i]], axis=0)
            for k in (2, 1, 3, 0):
                dst_x = lax.rem(x + k, RING)
                acc = dot(xs, wgu[dst_x])
                if k == 0:
                    own[i] = acc
                else:
                    gp[i, k - 1] = acc.astype(BF16)
                    send(gp.at[i, k - 1], hr.at[i, k - 1], G_S, g_recv.at[i], xdev(k))

    def second(i):
        with scope("gwait%d" % i):
            wait_bytes(hr.at[i], g_recv.at[i])
        with scope("second%d" % i):
            total = own[i]
            for k in range(RING - 1):
                total = total + hr[i, k].astype(F32)
            g = total[:, :inner]
            u = total[:, inner:]
            part = H.at[i, :, cols(x * inner, inner)]
            part[...] = (g / (1.0 + jnp.exp(-g)) * u).astype(BF16)
            for k in (2, 1, 3):
                send(part, part, H_S, h_recv.at[i], xdev(k))

    def hwait(i):
        with scope("hwait%d" % i):
            wait_bytes(H.at[i, :, pl.ds(0, (RING - 1) * inner)], h_recv.at[i])

    def dwait(q):
        with scope("dwait%d" % q):
            wait_bytes(wd.at[pl.ds(0, (RING - 1) * inner), pl.ds(*out[q])], wd_recv.at[q])
            w_loc[2 + q].wait()

    def down(i, q):
        o, w = out[q]
        return dot(H[i], wd[:, pl.ds(o, w)])

    def rsend(buf, into, q, rsem):
        o, w = out[q]
        for j, k in ((0, UP), (1, DOWN)):
            send(buf.at[pl.ds(j * half, half), pl.ds(o, w)], into.at[j, :, pl.ds(o, w)], R_S, rsem, zdev(k))

    def near(q):
        o, w = out[q]
        with scope("near%d" % q):
            pnear[:, pl.ds(o, w)] = down(N, q).astype(BF16)
            rsend(pnear, rdir, q, ro_recv.at[q])

    def far(q):
        o, w = out[q]
        with scope("far%d" % q):
            pfar[:, pl.ds(o, w)] = down(F, q).astype(BF16)
            rsend(pfar, rfar, q, rf_recv.at[q])

    def combine(q):
        o, w = out[q]
        sl = pl.ds(o, w)
        with scope("comb%d" % q):
            part = down(M, q)
        with scope("S1w%d" % q):
            wait_bytes(X.at[pl.ds(0, 2 * half), sl], rf_recv.at[q])
        for j in range(2):
            pcomb[pl.ds(j * half, half), sl] = (part[j * half:(j + 1) * half] + rfar[j, :, sl].astype(F32)).astype(BF16)
        rsend(pcomb, rcomb, q, ro_recv.at[q])

    def finish(q):
        o, w = out[q]
        sl = pl.ds(o, w)
        mine = down(O, q)
        with scope("S3w%d" % q):
            wait_bytes(X.at[pl.ds(0, 4 * half), sl], ro_recv.at[q])
        y_lo = mine[:half] + rcomb[0, :, sl].astype(F32) + rdir[1, :, sl].astype(F32)
        y_hi = mine[half:] + rcomb[1, :, sl].astype(F32) + rdir[0, :, sl].astype(F32)
        y = jnp.concatenate([y_lo.astype(BF16), y_hi.astype(BF16)], axis=0)
        sp = pl.ds(o, packed(w))
        sr[:, sp] = pack(p2t_ref, y)
        for k in range(1, n_ep):
            dst_e = lax.rem(ep + k, n_ep)
            send(sr.at[rows(dst_e * 16, 16), sp], rr.at[rows(ep * 16, 16), sp], C_S, c_recv.at[q], edev(k))
        rr[rows(ep * 16, 16), sp] = sr[rows(ep * 16, 16), sp]

    def give_back(q):
        o, w = out[q]
        sl = pl.ds(o, w)
        with scope("RBw%d" % q):
            wait_bytes(rr.at[pl.ds(0, others), pl.ds(o, packed(w))], c_recv.at[q])
        ts[:, sl] = unpack(p1t_ref, rr[:, pl.ds(o, packed(w))], w)
        for k in (2, 1, 3):
            dst_x = lax.rem(x + k, RING)
            send(ts.at[rows(dst_x * slots, slots), sl], ret_ref.at[:, cols(x * D4 + o, w)], E_S, d_recv.at[q], xdev(k))
        ret_ref[:, cols(x * D4 + o, w)] = ts[rows(x * slots, slots), sl]

    first(N)
    with scope("zfwait"):
        for q in range(C):
            zwait(zf_recv.at[q], q, 2)
    first(F)
    second(N)
    second(F)
    send_down(1)
    send_down(2)
    hwait(N)
    dwait(0)
    near(0)
    hwait(F)
    far(0)
    with scope("zmwait"):
        for q in range(C):
            zwait(zm_recv.at[q], q, 2)
    first(M)
    for q in range(3, Q):
        send_down(q)
    for q in (1, 2):
        dwait(q)
        near(q)
        far(q)
    second(M)
    first(O)
    for q in range(3, Q):
        dwait(q)
        far(q)
    second(O)
    hwait(M)
    combine(0)
    combine(1)
    for q in range(3, Q):
        near(q)
    combine(2)
    combine(3)
    hwait(O)
    for q in range(Q):
        finish(q)
    for q in range(Q):
        give_back(q)
    for q, (o, w) in enumerate(out):
        with scope("RAw%d" % q):
            wait_bytes(ts.at[pl.ds(0, (RING - 1) * slots), pl.ds(o, w)], d_recv.at[q])
        for j in range(RING):
            sl = pl.ds(j * D4 + o, w)
            mixed_ref[:, sl] = dot(scal_ref[...], ret_ref[:, sl]).astype(BF16)
    with scope("sends"):
        for group, ref in ((A_S, bs), (W_S, wgu.at[pl.ds(0, RING - 1)]),
                           (D_S, wd.at[pl.ds(0, (RING - 1) * inner), :]),
                           (B_S, sb.at[pl.ds(0, others), pl.ds(0, sum(packed(w) for _, w in into))]), (Z_S, X.at[pl.ds(0, 6 * half), :]),
                           (G_S, hr), (H_S, H.at[:, :, pl.ds(0, (RING - 1) * inner)]),
                           (R_S, X.at[pl.ds(0, 6 * half), :]), (C_S, sr.at[pl.ds(0, others), pl.ds(0, sum(packed(w) for _, w in out))]),
                           (E_S, ts.at[pl.ds(0, (RING - 1) * slots), :])):
            wait_bytes(ref, send_sem.at[group])


def body(tokens, expert_ids, gate_q, w_gate, w_up, w_down):
    n_ep = lax.axis_size("ep")
    T, width = tokens.shape
    D4 = width // RING
    slots = n_ep * CAP
    R = slots * RING
    inner = w_down.shape[1]
    per = CAP * RING

    p1 = np.zeros((1 + CAP, n_ep * 16, R), np.float32)
    p2 = np.zeros((1 + CAP, R, n_ep * 16), np.float32)
    for e in range(n_ep):
        for s in range(RING):
            for q in range(CAP):
                j = s * CAP + q
                p1[0, e * 16 + j, s * slots + e * CAP + q] = 1
                p1[1 + q, e * 16 + per + s, s * slots + e * CAP + q] = 1
                p2[0, e * per + j, e * 16 + j] = 1
                p2[1 + q, e * per + j, e * 16 + per + s] = 1
    consts = [jnp.asarray(m, BF16) for m in (p1, p1.transpose(0, 2, 1), p2, p2.transpose(0, 2, 1))]

    vm = pl.BlockSpec(memory_space=pltpu.VMEM)
    anyspec = pl.BlockSpec(memory_space=pl.ANY)
    V = pltpu.VMEM
    DMA = pltpu.SemaphoreType.DMA
    half = R // 2
    C, Q = len(CIN), len(CHUNKS)
    scratch = [
        V((slots, width), BF16), V((T, slots), BF16),
        V((expert_ids.shape[1], T), jnp.int32), V((expert_ids.shape[1], T), jnp.int32),
    ] + [V(m.shape, BF16) for m in consts] + [
        V((T, width), BF16),
        V((3, slots, D4), BF16),
        V((R, D4), BF16),
        V((n_ep * 16, D4), BF16),
        V((n_ep * 16, D4), BF16),
        V((RING * R, D4), BF16),
        V((RING, D4, 2 * inner), BF16),
        V((RING * inner, D4), BF16),
        V((RING, 3, R, 2 * inner), BF16),
        V((RING, R, 2 * inner), F32),
        V((RING, 3, R, 2 * inner), BF16),
        V((RING, R, RING * inner), BF16),
        V((R, D4), BF16),
        V((R, D4), BF16),
        V((R, D4), BF16),
        V((2, half, D4), BF16),
        V((2, half, D4), BF16),
        V((2, half, D4), BF16),
        V((n_ep * 16, D4), BF16),
        V((n_ep * 16, D4), BF16),
        V((R, D4), BF16),
        DMA((9 + Q,)), DMA((10,)), DMA(()), DMA((Q,)), DMA((C,)), DMA((C,)), DMA((C, 2)), DMA((C,)), DMA((C,)),
        DMA((4,)), DMA((4,)), DMA((Q,)), DMA((Q,)), DMA((Q,)), DMA((Q,)),
    ]
    return pl.pallas_call(
        kernel,
        out_shape=pltpu.VMEM((T, width), BF16),
        in_specs=[anyspec] * 10,
        out_specs=vm,
        scratch_shapes=scratch,
        compiler_params=pltpu.CompilerParams(collective_id=0, has_side_effects=True, vmem_limit_bytes=60 * 1024 * 1024),
        name="experts",
    )(expert_ids.T, gate_q.T, *consts, tokens, w_gate, w_up, w_down)


def solution(mesh):
    in_specs = (
        P(("ep", "etp"), None),
        P(("ep", "etp"), None),
        P(("ep", "etp"), None),
        P("ep", None, "etp"),
        P("ep", None, "etp"),
        P("ep", "etp", None),
    )
    out_specs = P(("ep", "etp"), None)
    return jax.shard_map(body, mesh=mesh, in_specs=in_specs, out_specs=out_specs, check_vma=False)
```
